8 devices in a mesh: m: 1 (over z), kk: 2 (over y), g: 4 (over x, core).
Axes of the slice: x: 2, y: 2, z: 1, core: 2. Of those that a mesh axis runs over, the one named last changes fastest.
Arguments:
- a_mat: bfloat16 [8, 4096, 14336], P(None, ('m', 'g'), 'kk')
Outputs:
- output: float32 [4, 3, 8, 1024, 1024], P(('m', 'g'))
All inputs are finite; a program needn't handle non-finite values.
Results may differ from the reference program's by a relative error of at most 0.001.
Values are sent between devices in bfloat16 or wider.
A program may use at most 1 GiB of HBM per device.

```python
import jax
import jax.numpy as jnp
from jax import lax

ROWS = 4096
COLS = 14336
LAYERS = 8
GROUP = 4

BLOCK = ROWS // GROUP
SLOTS = GROUP // 2 + 1


def assignment_table(groups):
    slot_count = groups // 2 + 1
    log_two = groups.bit_length() - 1
    side_len = 2 ** (log_two // 2)
    dup_count = groups // (side_len * side_len)
    grp_width = groups // side_len
    piece_len = max(1, grp_width // (2 * dup_count))
    pair_lists = [[] for device_no in range(groups)]
    block_sets = [set() for device_no in range(groups)]
    spill_pairs = []
    for upper_grp in range(side_len):
        for lower_grp in range(upper_grp):
            for left_row in range(upper_grp * grp_width, (upper_grp + 1) * grp_width):
                part_no = (left_row % grp_width) // piece_len
                if part_no < dup_count:
                    target = dup_count * (upper_grp * side_len + lower_grp) + part_no
                else:
                    target = dup_count * (lower_grp * side_len + upper_grp) + part_no - dup_count
                for right_row in range(lower_grp * grp_width, (lower_grp + 1) * grp_width):
                    pair_lists[target].append((left_row, right_row))
                    block_sets[target].update([left_row, right_row])
    for diag_grp in range(side_len):
        first_dev = dup_count * (diag_grp * side_len + diag_grp)
        for left_row in range(diag_grp * grp_width, (diag_grp + 1) * grp_width):
            for right_row in range(diag_grp * grp_width, left_row + 1):
                target = -1
                for copy_no in range(dup_count):
                    if target < 0 and len(pair_lists[first_dev + copy_no]) < slot_count:
                        target = first_dev + copy_no
                if target < 0:
                    spill_pairs.append((left_row, right_row))
                else:
                    pair_lists[target].append((left_row, right_row))
                    block_sets[target].update([left_row, right_row])
    for (left_row, right_row) in spill_pairs:
        best_score = (3, groups + 1, groups)
        for device_no in range(groups):
            if len(pair_lists[device_no]) < slot_count:
                growth = len(set([left_row, right_row]) - block_sets[device_no])
                cand_score = (growth, len(pair_lists[device_no]), device_no)
                best_score = min(best_score, cand_score)
        target = best_score[2]
        pair_lists[target].append((left_row, right_row))
        block_sets[target].update([left_row, right_row])
    return pair_lists, block_sets


def slot_tables(groups):
    pair_lists = assignment_table(groups)[0]
    slot_count = groups // 2 + 1
    left_rows = []
    right_rows = []
    live_flags = []
    for device_no in range(groups):
        own_pairs = pair_lists[device_no]
        left_rows.append([own_pairs[slot_no][0] if slot_no < len(own_pairs) else 0 for slot_no in range(slot_count)])
        right_rows.append([own_pairs[slot_no][1] if slot_no < len(own_pairs) else 0 for slot_no in range(slot_count)])
        live_flags.append([1 if slot_no < len(own_pairs) else 0 for slot_no in range(slot_count)])
    return left_rows, right_rows, live_flags


def setup_inputs(seed: int = 0, part: int = 0) -> dict:
    base_key = jax.random.fold_in(jax.random.key(seed), part)
    draw_key, scale_key = jax.random.split(base_key)
    values = jax.random.normal(draw_key, (LAYERS, GROUP, BLOCK, COLS), jnp.float32)
    block_scale = jnp.exp(jax.random.uniform(scale_key, (LAYERS, GROUP, 1, 1), jnp.float32, -0.35, 0.35))
    values = values * block_scale * (COLS ** -0.25)
    return {"a_mat": values.reshape(LAYERS, ROWS, COLS).astype(jnp.bfloat16)}


def reference(a_mat):
    left_rows, right_rows, live_flags = slot_tables(GROUP)

    def one_slot(slot_args):
        left_no, right_no, live_flag = slot_args
        left_blk = lax.dynamic_slice_in_dim(a_mat, left_no * BLOCK, BLOCK, axis=1).astype(jnp.float32)
        right_blk = lax.dynamic_slice_in_dim(a_mat, right_no * BLOCK, BLOCK, axis=1).astype(jnp.float32)
        product = jnp.einsum("lbk,lck->lbc", left_blk, right_blk)
        return jnp.where(live_flag == 1, product, jnp.zeros_like(product))

    blocks = lax.map(one_slot, (jnp.array(left_rows, jnp.int32).reshape(-1), jnp.array(right_rows, jnp.int32).reshape(-1), jnp.array(live_flags, jnp.int32).reshape(-1)))
    return blocks.reshape(GROUP, SLOTS, LAYERS, BLOCK, BLOCK)
```

```python
import functools

import jax
import jax.numpy as jnp
from jax import lax
from jax.experimental import pallas as pl
from jax.experimental.pallas import tpu as pltpu
from jax.sharding import PartitionSpec as P

MESH = pl.DeviceIdType.MESH
LANE = 128
AHEAD = 3
LEAD = 3


class Sizes:
    def __init__(self, layers, rows, cols):
        self.layers, self.rows, self.cols = layers, rows, cols
        self.half = layers // 2
        self.tile = rows // 2
        self.sub = self.tile // LANE
        self.full = self.sub * self.tile
        self.diag = self.sub * (self.sub + 1) // 2 * LANE
        self.own = 2 * self.diag + self.full
        self.mid = 4 * self.full
        self.part = 2 * self.full
        self.chunks = 2 * self.half
        self.depth = cols // 4 if cols % (4 * LANE) == 0 else cols


def exchange_kernel(sz, a, r, lp, rp, psd, psm, rsd, rsm, pc, rb, co, v, acc, stage, ba, bb,
                    load_sem, xs, xr, ls, lr, ds, dr, ss, sr, rss, rsr, cs, cr, fs):
    y = lax.axis_index("kk")
    g = lax.axis_index("g")
    x = g // 2
    c = g % 2
    away = c == x
    home = c != x
    layers, half, chunks = sz.layers, sz.half, sz.chunks

    to_x = {"g": (g + 2) % 4}
    to_core = {"g": 2 * x + 1 - c}
    to_y = {"kk": 1 - y}

    def remote(src, dst, send, recv, where):
        return pltpu.make_async_remote_copy(src_ref=src, dst_ref=dst, send_sem=send, recv_sem=recv, device_id=where,
                                            device_id_type=MESH)

    def x_in(q):
        j, h = q // 2, q % 2
        return remote(a.at[half * (1 - x) + j, h], r.at[j, h], xs.at[q], xr.at[q], to_x)

    def core_in(m):
        return remote(a.at[m], lp.at[m], ls.at[m], lr.at[m], to_core)

    def core_r(q):
        j, h = q // 2, q % 2
        return remote(r.at[j, h], rp.at[j, h], ds.at[q], dr.at[q], to_core)

    def send_diag(k, m):
        return remote(psd.at[k, m], rsd.at[k, m], ss.at[k, m], sr.at[k, m], to_y)

    def send_mid(m):
        return remote(psm.at[m], rsm.at[m], ss.at[2, m], sr.at[2, m], to_y)

    def send_part(q):
        src = pc.at[q, pl.ds(pl.multiple_of((1 - y) * sz.part, LANE), sz.part)]
        return remote(src, rb.at[q], rss.at[q], rsr.at[q], to_y)

    def send_sum(q):
        where = {"kk": jnp.where(home, 1 - y, y), "g": jnp.where(home, g, (g + 2) % 4)}
        return remote(co.at[x, q, y], co.at[x, q, y], cs.at[q], cr.at[jnp.where(home, 0, 1), q], where)

    def from_x(q):
        return remote(co.at[1 - x, q, y], co.at[1 - x, q, y], fs.at[q], cr.at[1, q], to_x)

    def forward(q):
        return remote(co.at[1 - x, q, y], co.at[1 - x, q, y], fs.at[q], cr.at[2, q], to_y)

    def load(src, dst, k):
        pltpu.make_async_copy(src, dst, load_sem.at[k]).start()

    def loaded(dst, k):
        pltpu.make_async_copy(dst, dst, load_sem.at[k]).wait()

    def store(src, dst):
        copy = pltpu.make_async_copy(src, dst, load_sem.at[6])
        copy.start()
        copy.wait()

    def product(left, right):
        acc[...] = jnp.zeros_like(acc)

        def step(k, carry):
            cols = pl.ds(pl.multiple_of(k * sz.depth, LANE), sz.depth)
            acc[...] += lax.dot_general(v[left, :, cols], v[right, :, cols], (((1,), (1,)), ((), ())),
                                        preferred_element_type=jnp.float32)
            return carry

        lax.fori_loop(0, sz.cols // sz.depth, step, 0)

    def put_full(row):
        for s in range(sz.sub):
            rows = pl.ds(pl.multiple_of(row + s * sz.tile, LANE), sz.tile)
            stage[rows, :] = acc[:, s * LANE:(s + 1) * LANE]

    def put_diag(row):
        n = 0
        for i in range(sz.sub):
            for k in range(i + 1):
                rows = pl.ds(pl.multiple_of(row + n * LANE, LANE), LANE)
                stage[rows, :] = acc[i * LANE:(i + 1) * LANE, k * LANE:(k + 1) * LANE]
                n += 1

    def same_chip(m):
        load(a.at[m, 0], v.at[0], 0)
        load(a.at[m, 1], v.at[1], 1)
        core_in(m).wait_recv()
        load(lp.at[m, 0], v.at[2], 2)
        load(lp.at[m, 1], v.at[3], 3)

        def diagonal(k):
            def one(d, carry):
                product(2 * k + d, 2 * k + d)
                put_diag(d * sz.diag)
                return carry

            lax.fori_loop(0, 2, one, 0)
            product(2 * k + 1, 2 * k)
            put_full(2 * sz.diag)
            store(stage.at[pl.ds(0, sz.own)], psd.at[k, m])
            send_diag(k, m).start()

        def middle(n, carry):
            i, k = n // 2, n % 2
            product(i + 2 * (1 - x), k + 2 * x)
            put_full(n * sz.full)
            return carry

        def diagonals(k, carry):
            for n in range(2):
                @pl.when(k == 0)
                def _():
                    loaded(v.at[n], n)
            diagonal(k)

            @pl.when(k == 0)
            def _():
                for n in range(2, 4):
                    loaded(v.at[n], n)
            return carry

        lax.fori_loop(0, 2, diagonals, 0)
        lax.fori_loop(0, 4, middle, 0)
        store(stage, psm.at[m])
        send_mid(m).start()

    def cross(q):
        j, h = q // 2, q % 2
        x_in(q).wait_recv()

        @pl.when(x == 0)
        def _():
            @pl.when(home & (h == 0))
            def _():
                core_in(j).wait_recv()

            own, other = 2 * c, 2 - 2 * c
            for n in range(2):
                load(a.at[j, n], v.at[own + n], n)
                load(lp.at[j, n], v.at[other + n], 2 + n)
            load(r.at[j, h], v.at[4], 4)
            for n in range(2):
                loaded(v.at[own + n], n)
                loaded(v.at[other + n], 2 + n)
            loaded(v.at[4], 4)

        @pl.when(x == 1)
        def _():
            core_r(q).start()
            for n in range(2):
                load(a.at[half + j, n], v.at[4 + n], n)
            load(r.at[j, h], v.at[c], 2)
            core_r(q).wait_recv()
            load(rp.at[j, h], v.at[1 - c], 3)
            for n in range(2):
                loaded(v.at[4 + n], n)
            loaded(v.at[c], 2)
            loaded(v.at[1 - c], 3)

        def one(n, carry):
            i, t = n // 2, n % 2
            product(4 + x * t, jnp.where(x == 0, n, i))
            put_full(n * sz.full)
            return carry

        lax.fori_loop(0, 4, one, 0)
        store(stage, pc.at[q])
        send_part(q).start()

    def add(q):
        send_part(q).wait_recv()
        load(pc.at[q, pl.ds(pl.multiple_of(y * sz.part, LANE), sz.part)], ba, 0)
        load(rb.at[q], bb, 1)
        loaded(ba, 0)
        loaded(bb, 1)
        ba[...] += bb[...]
        store(ba, co.at[x, q, y])
        send_sum(q).start()

    def pass_on(q):
        from_x(q).wait_recv()
        forward(q).start()

    barrier = pltpu.get_barrier_semaphore()
    for where in (to_x, to_core, to_y):
        pl.semaphore_signal(barrier, inc=1, device_id=where, device_id_type=MESH)
    pl.semaphore_wait(barrier, 3)

    def loop(lo, hi, f):
        def body(n, carry):
            f(n)
            return carry

        lax.fori_loop(lo, hi, body, 0)

    loop(0, AHEAD, lambda q: x_in(q).start())

    @pl.when(home)
    def _():
        loop(0, layers, lambda m: core_in(m).start())

    @pl.when(away & (x == 0))
    def _():
        loop(0, half, lambda m: core_in(m).start())

    @pl.when(away)
    def _():
        loop(0, LEAD, same_chip)

    def round_(q):
        cross(q)

        @pl.when(away & (q < layers - LEAD))
        def _():
            same_chip(q + LEAD)

        add(q)

        @pl.when(q < chunks - AHEAD)
        def _():
            x_in(q + AHEAD).start()

        @pl.when(home & (q >= 2))
        def _():
            pass_on(q - 2)

    loop(0, chunks, round_)

    @pl.when(home)
    def _():
        loop(chunks - 2, chunks, pass_on)
        loop(0, layers, lambda m: core_in(m).wait_send())

        def end(q):
            send_sum(q).wait_recv()
            forward(q).wait_recv()
            forward(q).wait_send()

        loop(0, chunks, end)

    @pl.when(away & (x == 0))
    def _():
        loop(0, half, lambda m: core_in(m).wait_send())

    @pl.when(x == 1)
    def _():
        loop(0, chunks, lambda q: core_r(q).wait_send())

    @pl.when(away)
    def _():
        def end(m):
            for k in range(2):
                send_diag(k, m).wait()
            send_mid(m).wait()

        loop(0, layers, end)

    def sent(q):
        x_in(q).wait_send()
        send_part(q).wait_send()
        send_sum(q).wait_send()

    loop(0, chunks, sent)


def exchange(sz, a):
    f32, bf16 = jnp.float32, jnp.bfloat16
    dma = pltpu.SemaphoreType.DMA
    halves = (2, sz.tile, sz.cols)
    outs = [
        ((sz.half,) + halves, bf16),
        ((sz.layers,) + halves, bf16),
        ((sz.half,) + halves, bf16),
        ((2, sz.layers, sz.own, LANE), f32),
        ((sz.layers, sz.mid, LANE), f32),
        ((2, sz.layers, sz.own, LANE), f32),
        ((sz.layers, sz.mid, LANE), f32),
        ((sz.chunks, 2 * sz.part, LANE), f32),
        ((sz.chunks, sz.part, LANE), f32),
        ((2, sz.chunks, 2, sz.part, LANE), f32),
    ]
    n, q = sz.layers, sz.chunks
    res = pl.pallas_call(
        functools.partial(exchange_kernel, sz),
        name="exchange",
        out_shape=[jax.ShapeDtypeStruct(s, d) for s, d in outs],
        in_specs=[pl.BlockSpec(memory_space=pl.ANY)],
        out_specs=[pl.BlockSpec(memory_space=pl.ANY)] * len(outs),
        scratch_shapes=[
            pltpu.VMEM((6, sz.tile, sz.cols), bf16),
            pltpu.VMEM((sz.tile, sz.tile), f32),
            pltpu.VMEM((sz.mid, LANE), f32),
            pltpu.VMEM((sz.part, LANE), f32),
            pltpu.VMEM((sz.part, LANE), f32),
            dma((7,)), dma((q,)), dma((q,)), dma((n,)), dma((n,)), dma((q,)), dma((q,)),
            dma((3, n)), dma((3, n)), dma((q,)), dma((q,)), dma((q,)), dma((3, q)), dma((q,)),
        ],
        compiler_params=pltpu.CompilerParams(collective_id=0, has_side_effects=True, vmem_limit_bytes=60 * 2**20),
    )(a)
    return res[3], res[5], res[4], res[6], res[9]


def assemble_kernel(sz, role, psd0, rsd0, psm, rsm, psd1, rsd1, co, out):
    away = role[0] == 1
    x = role[1]
    t, sub = sz.tile, sz.sub
    slot = pl.program_id(1)
    m = pl.program_id(0)

    def diagonal(mine, theirs):
        for d in range(2):
            n = 0
            for i in range(sub):
                for k in range(i + 1):
                    rows = slice(d * sz.diag + n * LANE, d * sz.diag + (n + 1) * LANE)
                    s = mine[0, 0, rows, :] + theirs[0, 0, rows, :]
                    lo, hi = d * t + i * LANE, d * t + k * LANE
                    out[0, 0, lo:lo + LANE, hi:hi + LANE] = s
                    if i != k:
                        out[0, 0, hi:hi + LANE, lo:lo + LANE] = s.T
                    n += 1
        for k in range(sub):
            for i in range(sub):
                rows = slice(2 * sz.diag + k * t + i * LANE, 2 * sz.diag + k * t + (i + 1) * LANE)
                s = mine[0, 0, rows, :] + theirs[0, 0, rows, :]
                lo, hi = t + i * LANE, k * LANE
                out[0, 0, lo:lo + LANE, hi:hi + LANE] = s
                out[0, 0, hi:hi + LANE, lo:lo + LANE] = s.T

    @pl.when(away & (slot == 2 * x))
    def _():
        diagonal(psd0, rsd0)

    @pl.when(away & (slot == 2 - 2 * x))
    def _():
        diagonal(psd1, rsd1)

    @pl.when(away & (slot == 1))
    def _():
        for n in range(4):
            i, k = n // 2, n % 2
            for s in range(sub):
                rows = slice(n * sz.full + s * t, n * sz.full + (s + 1) * t)
                col = k * t + s * LANE
                out[0, 0, i * t:(i + 1) * t, col:col + LANE] = psm[0, rows, :] + rsm[0, rows, :]

    def cross(first):
        for h in range(2):
            for n in range(2):
                i, k = (h, n) if first else (n, h)
                for s in range(sub):
                    rows = slice(n * sz.full + s * t, n * sz.full + (s + 1) * t)
                    col = k * t + s * LANE
                    out[0, 0, i * t:(i + 1) * t, col:col + LANE] = co[0, h, 0, rows, :]

    @pl.when((role[0] == 0) & (slot < 2) & (m < sz.half))
    def _():
        cross(True)

    @pl.when((role[0] == 0) & (slot < 2) & (m >= sz.half))
    def _():
        cross(False)

    @pl.when((role[0] == 0) & (slot == 2))
    def _():
        out[...] = jnp.zeros_like(out)


def assemble(sz, role, psd, rsd, psm, rsm, co):
    def diag_at(k):
        return lambda m, slot, role: (k, m * role[0], 0, 0)

    def mid_at(m, slot, role):
        return (m * role[0], 0, 0)

    def cross_at(m, slot, role):
        home = 1 - role[0]
        return (home * (m // sz.half), home * (m % sz.half), home * jnp.minimum(slot, 1), 0, 0)

    diag = (1, 1, sz.own, LANE)
    mid = (1, sz.mid, LANE)
    return pl.pallas_call(
        functools.partial(assemble_kernel, sz),
        name="assemble",
        out_shape=jax.ShapeDtypeStruct((3, sz.layers, sz.rows, sz.rows), jnp.float32),
        grid_spec=pltpu.PrefetchScalarGridSpec(
            num_scalar_prefetch=1,
            grid=(sz.layers, 3),
            in_specs=[
                pl.BlockSpec(diag, diag_at(0)), pl.BlockSpec(diag, diag_at(0)),
                pl.BlockSpec(mid, mid_at), pl.BlockSpec(mid, mid_at),
                pl.BlockSpec(diag, diag_at(1)), pl.BlockSpec(diag, diag_at(1)),
                pl.BlockSpec((1, 2, 1, sz.part, LANE), cross_at),
            ],
            out_specs=pl.BlockSpec((1, 1, sz.rows, sz.rows), lambda m, slot, role: (slot, m, 0, 0)),
        ),
        compiler_params=pltpu.CompilerParams(vmem_limit_bytes=60 * 2**20),
    )(role, psd, rsd, psm, rsm, psd, rsd, co)


def solution(mesh):
    def local_part(a_loc):
        sz = Sizes(*a_loc.shape)
        g = lax.axis_index("g")
        x, c = g // 2, g % 2
        role = jnp.stack([jnp.where(c == x, 1, 0), x]).astype(jnp.int32)
        parts = exchange(sz, a_loc.reshape(sz.layers, 2, sz.tile, sz.cols))
        return assemble(sz, role, *parts)[None]

    return jax.shard_map(local_part, mesh=mesh, in_specs=(P(None, ("m", "g"), "kk"),), out_specs=P(("m", "g"), None, None, None, None), check_vma=False)
```

```python
import functools

import jax
import jax.numpy as jnp
from jax import lax
from jax.experimental import pallas as pl
from jax.experimental.pallas import tpu as pltpu
from jax.sharding import PartitionSpec as P

MESH = pl.DeviceIdType.MESH
LANE = 128
CHUNKS = 4

PLAN = (
    (
        "SISIXSAISISXXIISSASXSSXISASSXIAXISAAXAXIXISSISAISS",
        "SISXXSXSIAXAAXAAISXAAA",
    ),
    (
        "IIXIIXIXXAIFAIXAFIAXIIAXAXIIAIXIXFFXAFXFAAAIAXFIFF",
        "XAXAFFAFXFFFFA",
    ),
    (
        "IIRIRXIAIXIRIRAXIRRXXFFAIAAIIXRRRFIFRIAXIAFFIXRRAX",
        "AXXRFFIAAXRRAXFFXFXAFAAFRFXFAF",
    ),
    (
        "SSSISRSISRXSASSIXASRXRISRISAXSIAISXSISRIXAISSRIIIX",
        "ASRSXRSRSXSXASAAIRAIIXRRXXRARXAXAARAXA",
    ),
)
STEPS = "IRXAFS"
WORD = 10


def plan_words():
    rows = []
    for pieces in PLAN:
        codes, count, kept = [], 0, False
        for step in "".join(pieces):
            codes.append(STEPS.index(step) + 1)
            if step == "S":
                codes[-1] += kept and count % 3 > 0
                count, kept = count + 1, True
            kept = kept and step != "X"
        rows.append([sum(code << (3 * k) for k, code in enumerate(codes[n:n + WORD])) for n in range(0, len(codes), WORD)])
    longest = max(len(row) for row in rows)
    return [row + [0] * (longest - len(row)) for row in rows]


class Sizes:
    def __init__(self, layers, rows, cols):
        self.layers, self.rows, self.cols = layers, rows, cols
        self.half = layers // 2
        self.tile = rows // 2
        self.piece = rows // CHUNKS
        self.sub = self.tile // LANE
        self.full = self.sub * self.tile
        self.pairs = (self.sub + 1) // 2
        self.low = self.sub * (self.sub - 1) // 2
        self.diag = (self.low + self.pairs) * LANE + (self.pairs + 7) // 8 * 8
        self.own = 2 * self.diag + self.full
        self.mid = 4 * self.full
        self.flat = self.piece // LANE * self.tile
        self.part = 2 * self.flat
        self.chunks = CHUNKS * self.half
        self.depth = cols // 4 if cols % (4 * LANE) == 0 else cols


def triangles():
    row = lax.broadcasted_iota(jnp.int32, (LANE, LANE), 0)
    col = lax.broadcasted_iota(jnp.int32, (LANE, LANE), 1)
    return row >= col, row == col


def exchange_kernel(sz, a, r, lp, rp, psd, psm, rsd, rsm, pc, rb, co, v, acc, stage, ba, bb,
                    load_sem, xs, xr, ls, lr, ds, dr, ss, sr, rss, rsr, cs, cr, fs):
    y = lax.axis_index("kk")
    g = lax.axis_index("g")
    x = g // 2
    c = g % 2
    away = c == x
    home = c != x
    layers, half, chunks = sz.layers, sz.half, sz.chunks

    to_x = {"g": (g + 2) % 4}
    to_core = {"g": 2 * x + 1 - c}
    to_y = {"kk": 1 - y}

    def remote(src, dst, send, recv, where):
        return pltpu.make_async_remote_copy(src_ref=src, dst_ref=dst, send_sem=send, recv_sem=recv, device_id=where,
                                            device_id_type=MESH)

    def chunk(ref, q):
        return ref.at[q // CHUNKS, pl.ds(pl.multiple_of(q % CHUNKS * sz.piece, sz.piece), sz.piece)]

    def x_in(q):
        return remote(chunk(a, half * (1 - x) * CHUNKS + q), chunk(r, q), xs.at[q], xr.at[q], to_x)

    def core_in(m):
        return remote(a.at[m], lp.at[m], ls.at[m], lr.at[m], to_core)

    def core_r(q):
        return remote(chunk(r, q), chunk(rp, q), ds.at[q], dr.at[q], to_core)

    def send_diag(k, m, rows=None):
        src, dst = psd.at[k, m], rsd.at[k, m]
        if rows is not None:
            src, dst = src.at[rows], dst.at[rows]
        return remote(src, dst, ss.at[k, m], sr.at[k, m], to_y)

    def send_mid(m, rows=None):
        src, dst = psm.at[m], rsm.at[m]
        if rows is not None:
            src, dst = src.at[rows], dst.at[rows]
        return remote(src, dst, ss.at[2, m], sr.at[2, m], to_y)

    def send_part(q):
        src = pc.at[q, pl.ds(pl.multiple_of((1 - y) * sz.part, LANE), sz.part)]
        return remote(src, rb.at[q], rss.at[q], rsr.at[q], to_y)

    def send_sum(q):
        where = {"kk": jnp.where(home, 1 - y, y), "g": jnp.where(home, g, (g + 2) % 4)}
        return remote(co.at[x, q, y], co.at[x, q, y], cs.at[q], cr.at[jnp.where(home, 0, 1), q], where)

    def from_x(q):
        return remote(co.at[1 - x, q, y], co.at[1 - x, q, y], fs.at[q], cr.at[1, q], to_x)

    def forward(q):
        return remote(co.at[1 - x, q, y], co.at[1 - x, q, y], fs.at[q], cr.at[2, q], to_y)

    def load(src, dst, k):
        pltpu.make_async_copy(src, dst, load_sem.at[k]).start()

    def loaded(dst, k):
        pltpu.make_async_copy(dst, dst, load_sem.at[k]).wait()

    def store(src, dst):
        copy = pltpu.make_async_copy(src, dst, load_sem.at[4])
        copy.start()
        copy.wait()

    def block(n, rows=sz.rows):
        return v.at[pl.ds(pl.multiple_of(n, LANE), rows)]

    def product(left, right, width):
        acc[:, :width] = jnp.zeros((sz.tile, width), jnp.float32)

        def step(k, carry):
            cols = pl.ds(pl.multiple_of(k * sz.depth, LANE), sz.depth)
            lhs = v[pl.ds(pl.multiple_of(left, LANE), sz.tile), cols]
            rhs = v[pl.ds(pl.multiple_of(right, LANE), width), cols]
            acc[:, :width] += lax.dot_general(lhs, rhs, (((1,), (1,)), ((), ())), preferred_element_type=jnp.float32)
            return carry

        lax.fori_loop(0, sz.cols // sz.depth, step, 0)

    def put_strips(row, width):
        for s in range(width // LANE):
            rows = pl.ds(pl.multiple_of(row + s * sz.tile, 8), sz.tile)
            stage[rows, :] = acc[:, s * LANE:(s + 1) * LANE]

    def put_diag(row):
        def subtile(i, k):
            return acc[i * LANE:(i + 1) * LANE, k * LANE:(k + 1) * LANE]

        n = row
        for i in range(sz.sub):
            for k in range(i):
                stage[n:n + LANE, :] = subtile(i, k)
                n += LANE
        lower, equal = triangles()
        tail = row + (sz.low + sz.pairs) * LANE
        stage[tail:row + sz.diag, :] = jnp.zeros((row + sz.diag - tail, LANE), jnp.float32)
        for i in range(0, sz.sub, 2):
            if i + 1 < sz.sub:
                other = subtile(i + 1, i + 1)
                stage[n:n + LANE, :] = jnp.where(lower, subtile(i, i), other)
                stage[tail + i // 2:tail + i // 2 + 1, :] = jnp.sum(jnp.where(equal, other, 0.0), axis=0, keepdims=True)
            else:
                stage[n:n + LANE, :] = subtile(i, i)
            n += LANE

    def same_chip(n, kept):
        m, k = n // 3, n % 3

        def halves(ref, at):
            for d in range(2):
                load(ref.at[m, pl.ds(d * sz.tile, sz.tile)], block(at + d * sz.tile, sz.tile), d)

        @pl.when(k == 0)
        def _():
            halves(a, 0)

        @pl.when((k == 2) & (kept == 0))
        def _():
            halves(lp, sz.rows)

        @pl.when(k == 1)
        def _():
            core_in(m).wait_recv()

            @pl.when(kept == 0)
            def _():
                load(a.at[m], block(0), 2)
                loaded(block(0), 2)

            load(lp.at[m], block(sz.rows), 3)
            loaded(block(sz.rows), 3)

            def middle(i, carry):
                lhs, rhs = i // 2 * sz.tile + (1 - x) * sz.rows, i % 2 * sz.tile + x * sz.rows
                product(lhs, rhs, sz.tile)
                put_strips(i * sz.full, sz.tile)

                @pl.when(n == 1)
                def _():
                    rows = pl.ds(pl.multiple_of(i * sz.full, LANE), sz.full)
                    store(stage.at[rows], psm.at[m, rows])
                    send_mid(m, rows).start()
                return carry

            lax.fori_loop(0, 4, middle, 0)

            @pl.when(n > 1)
            def _():
                store(stage, psm.at[m])
                send_mid(m).start()

        @pl.when(k != 1)
        def _():
            which = k // 2
            base = which * sz.rows

            def piece(lo, size):
                @pl.when(n == 0)
                def _():
                    rows = pl.ds(lo, size)
                    store(stage.at[rows], psd.at[which, m, rows])
                    send_diag(which, m, rows).start()

            for d in range(2):
                @pl.when((k == 0) | (kept == 0))
                def _():
                    loaded(block(base + d * sz.tile, sz.tile), d)

                product(base + d * sz.tile, base + d * sz.tile, sz.tile)
                put_diag(d * sz.diag)
                piece(d * sz.diag, sz.diag)
            product(base + sz.tile, base, sz.tile)
            put_strips(2 * sz.diag, sz.tile)
            piece(2 * sz.diag, sz.full)

            @pl.when(n > 0)
            def _():
                store(stage.at[pl.ds(0, sz.own)], psd.at[which, m])
                send_diag(which, m).start()

    def relay(q):
        x_in(q).wait_recv()
        core_r(q).start()

    def cross(q):
        j = q // CHUNKS

        @pl.when(x == 0)
        def _():
            @pl.when(home & (q % CHUNKS == 0))
            def _():
                core_in(j).wait_recv()

            load(a.at[j], block(c * sz.rows), 0)
            load(lp.at[j], block((1 - c) * sz.rows), 1)
            x_in(q).wait_recv()
            load(chunk(r, q), block(2 * sz.rows, sz.piece), 2)
            loaded(block(c * sz.rows), 0)
            loaded(block((1 - c) * sz.rows), 1)
            loaded(block(2 * sz.rows, sz.piece), 2)

        @pl.when(x == 1)
        def _():
            load(a.at[half + j], block(2 * sz.rows), 0)
            load(chunk(r, q), block(c * sz.piece, sz.piece), 1)
            core_r(q).wait_recv()
            load(chunk(rp, q), block((1 - c) * sz.piece, sz.piece), 2)
            loaded(block(2 * sz.rows), 0)
            loaded(block(c * sz.piece, sz.piece), 1)
            loaded(block((1 - c) * sz.piece, sz.piece), 2)

        def one(n, carry):
            lhs = n * sz.tile * (1 - x) + (2 * sz.rows + n % 2 * sz.tile) * x
            rhs = 2 * sz.rows * (1 - x) + n // 2 * sz.piece * x
            product(lhs, rhs, sz.piece)
            put_strips(n * sz.flat, sz.piece)
            return carry

        lax.fori_loop(0, 4, one, 0)
        store(stage.at[pl.ds(0, 2 * sz.part)], pc.at[q])
        send_part(q).start()

    def add(q):
        load(pc.at[q, pl.ds(pl.multiple_of(y * sz.part, LANE), sz.part)], ba, 0)
        send_part(q).wait_recv()
        load(rb.at[q], bb, 1)
        loaded(ba, 0)
        loaded(bb, 1)
        ba[...] += bb[...]
        store(ba, co.at[x, q, y])
        send_sum(q).start()

    def pass_on(q):
        from_x(q).wait_recv()
        forward(q).start()

    barrier = pltpu.get_barrier_semaphore()
    for where in (to_x, to_core, to_y):
        pl.semaphore_signal(barrier, inc=1, device_id=where, device_id_type=MESH)
    pl.semaphore_wait(barrier, 3)

    def loop(lo, hi, f):
        def body(n, carry):
            f(n)
            return carry

        lax.fori_loop(lo, hi, body, 0)

    @pl.when(home)
    def _():
        loop(0, layers, lambda m: core_in(m).start())

    @pl.when(away & (x == 0))
    def _():
        loop(0, half, lambda m: core_in(m).start())

    steps = [lambda q: x_in(q).start(), relay, cross, add, pass_on]

    def word(n, done):
        code = jnp.int32(0)
        for device, words in enumerate(plan_words()):
            for k, value in enumerate(words):
                code = jnp.where((g == device) & (n == k), value, code)

        def digit(_, carry):
            code, done = carry[0], list(carry[1:])
            now = code % 8
            for k, step in enumerate(steps):
                pl.when(now == k + 1)(functools.partial(step, done[k]))
                done[k] += jnp.where(now == k + 1, 1, 0)
            pl.when(now > len(steps))(functools.partial(same_chip, done[-1], now - len(steps) - 1))
            done[-1] += jnp.where(now > len(steps), 1, 0)
            return (code // 8, *done)

        return lax.fori_loop(0, WORD, digit, (code, *done))[1:]

    lax.fori_loop(0, len(plan_words()[0]), word, (jnp.int32(0),) * (len(steps) + 1))

    @pl.when(home)
    def _():
        loop(0, layers, lambda m: core_in(m).wait_send())

        def end(q):
            send_sum(q).wait_recv()
            forward(q).wait_recv()
            forward(q).wait_send()

        loop(0, chunks, end)

    @pl.when(away & (x == 0))
    def _():
        loop(0, half, lambda m: core_in(m).wait_send())

    @pl.when(x == 1)
    def _():
        loop(0, chunks, lambda q: core_r(q).wait_send())

    @pl.when(away)
    def _():
        def end(m):
            for k in range(2):
                send_diag(k, m).wait()
            send_mid(m).wait()

        loop(0, layers, end)

    def sent(q):
        x_in(q).wait_send()
        send_part(q).wait_send()
        send_sum(q).wait_send()

    loop(0, chunks, sent)


def exchange(sz, a):
    f32, bf16 = jnp.float32, jnp.bfloat16
    dma = pltpu.SemaphoreType.DMA
    rows = (sz.rows, sz.cols)
    outs = [
        ((sz.half,) + rows, bf16),
        ((sz.layers,) + rows, bf16),
        ((sz.half,) + rows, bf16),
        ((2, sz.layers, sz.own, LANE), f32),
        ((sz.layers, sz.mid, LANE), f32),
        ((2, sz.layers, sz.own, LANE), f32),
        ((sz.layers, sz.mid, LANE), f32),
        ((sz.chunks, 2 * sz.part, LANE), f32),
        ((sz.chunks, sz.part, LANE), f32),
        ((2, sz.chunks, 2, sz.part, LANE), f32),
    ]
    n, q = sz.layers, sz.chunks
    res = pl.pallas_call(
        functools.partial(exchange_kernel, sz),
        name="exchange",
        out_shape=[jax.ShapeDtypeStruct(s, d) for s, d in outs],
        in_specs=[pl.BlockSpec(memory_space=pl.ANY)],
        out_specs=[pl.BlockSpec(memory_space=pl.ANY)] * len(outs),
        scratch_shapes=[
            pltpu.VMEM((3 * sz.rows, sz.cols), bf16),
            pltpu.VMEM((sz.tile, sz.tile), f32),
            pltpu.VMEM((sz.mid, LANE), f32),
            pltpu.VMEM((sz.part, LANE), f32),
            pltpu.VMEM((sz.part, LANE), f32),
            dma((5,)), dma((q,)), dma((q,)), dma((n,)), dma((n,)), dma((q,)), dma((q,)),
            dma((3, n)), dma((3, n)), dma((q,)), dma((q,)), dma((q,)), dma((3, q)), dma((q,)),
        ],
        compiler_params=pltpu.CompilerParams(collective_id=0, has_side_effects=True, vmem_limit_bytes=60 * 2**20),
    )(a)
    return res[3], res[5], res[4], res[6], res[9]


def assemble_kernel(sz, role, psd0, rsd0, psm, rsm, psd1, rsd1, co, out):
    away = role[0] == 1
    x = role[1]
    t, sub = sz.tile, sz.sub
    slot = pl.program_id(1)
    m = pl.program_id(0)

    lower, equal = triangles()

    def put(i, k, value):
        out[0, 0, i * LANE:(i + 1) * LANE, k * LANE:(k + 1) * LANE] = value

    def diagonal(mine, theirs):
        def total(row, size=LANE):
            return mine[0, 0, row:row + size, :] + theirs[0, 0, row:row + size, :]

        for d in range(2):
            row, first = d * sz.diag, d * sub
            tail = row + (sz.low + sz.pairs) * LANE
            for i in range(sub):
                for k in range(i):
                    s = total(row)
                    put(first + i, first + k, s)
                    put(first + k, first + i, s.T)
                    row += LANE
            for i in range(0, sub, 2):
                s = total(row)
                flip = s.T
                put(first + i, first + i, jnp.where(lower, s, flip))
                if i + 1 < sub:
                    line = jnp.broadcast_to(total(tail + i // 2, 1), (LANE, LANE))
                    other = jnp.where(equal, line, jnp.where(lower, flip, s))
                    put(first + i + 1, first + i + 1, other)
                row += LANE
        for k in range(sub):
            for i in range(sub):
                s = total(2 * sz.diag + k * t + i * LANE)
                put(sub + i, k, s)
                put(k, sub + i, s.T)

    @pl.when(away & (slot == 2 * x))
    def _():
        diagonal(psd0, rsd0)

    @pl.when(away & (slot == 2 - 2 * x))
    def _():
        diagonal(psd1, rsd1)

    @pl.when(away & (slot == 1))
    def _():
        for n in range(4):
            i, k = n // 2, n % 2
            for s in range(sub):
                rows = slice(n * sz.full + s * t, n * sz.full + (s + 1) * t)
                col = k * t + s * LANE
                out[0, 0, i * t:(i + 1) * t, col:col + LANE] = psm[0, rows, :] + rsm[0, rows, :]

    def cross(transposed):
        strips = sz.piece // LANE
        for h in range(CHUNKS):
            for n in range(2):
                for s in range(strips):
                    for i in range(sub):
                        row = n * sz.flat + s * t + i * LANE
                        value = co[0, h, 0, row:row + LANE, :]
                        across, along = h * strips + s, n * sub + i
                        if transposed:
                            put(across, along, value.T)
                        else:
                            put(along, across, value)

    @pl.when((role[0] == 0) & (slot < 2) & (m < sz.half))
    def _():
        cross(True)

    @pl.when((role[0] == 0) & (slot < 2) & (m >= sz.half))
    def _():
        cross(False)

    @pl.when((role[0] == 0) & (slot == 2))
    def _():
        out[...] = jnp.zeros_like(out)


def assemble(sz, role, psd, rsd, psm, rsm, co):
    def diag_at(k):
        return lambda m, slot, role: (k, m * role[0], 0, 0)

    def mid_at(m, slot, role):
        return (m * role[0], 0, 0)

    def cross_at(m, slot, role):
        home = 1 - role[0]
        return (home * (m // sz.half), home * (m % sz.half), home * jnp.minimum(slot, 1), 0, 0)

    diag = (1, 1, sz.own, LANE)
    mid = (1, sz.mid, LANE)
    return pl.pallas_call(
        functools.partial(assemble_kernel, sz),
        name="assemble",
        out_shape=jax.ShapeDtypeStruct((3, sz.layers, sz.rows, sz.rows), jnp.float32),
        grid_spec=pltpu.PrefetchScalarGridSpec(
            num_scalar_prefetch=1,
            grid=(sz.layers, 3),
            in_specs=[
                pl.BlockSpec(diag, diag_at(0)), pl.BlockSpec(diag, diag_at(0)),
                pl.BlockSpec(mid, mid_at), pl.BlockSpec(mid, mid_at),
                pl.BlockSpec(diag, diag_at(1)), pl.BlockSpec(diag, diag_at(1)),
                pl.BlockSpec((1, CHUNKS, 1, sz.part, LANE), cross_at),
            ],
            out_specs=pl.BlockSpec((1, 1, sz.rows, sz.rows), lambda m, slot, role: (slot, m, 0, 0)),
        ),
        compiler_params=pltpu.CompilerParams(vmem_limit_bytes=60 * 2**20),
    )(role, psd, rsd, psm, rsm, psd, rsd, co)


def solution(mesh):
    def local_part(a_loc):
        sz = Sizes(*a_loc.shape)
        g = lax.axis_index("g")
        x, c = g // 2, g % 2
        role = jnp.stack([jnp.where(c == x, 1, 0), x]).astype(jnp.int32)
        parts = exchange(sz, a_loc)
        return assemble(sz, role, *parts)[None]

    return jax.shard_map(local_part, mesh=mesh, in_specs=(P(None, ("m", "g"), "kk"),), out_specs=P(("m", "g"), None, None, None, None), check_vma=False)
```

```python
import functools

import jax
import jax.numpy as jnp
from jax import lax
from jax.experimental import pallas as pl
from jax.experimental.pallas import tpu as pltpu
from jax.sharding import PartitionSpec as P

MESH = pl.DeviceIdType.MESH
LANE = 128

SPLIT = ((14, 2), (4, 1))

PLAN = (
    (
        "ISSISXSSIIIIIXXASSIISSIAXSSIAAXSSSSIAXSXSXISAASIXX",
        "XSSXIAAIISXAAXAAISXSXXAAXAAA",
    ),
    (
        "IXIIIIIIAXXFIXIXXAIIXAAXAXIXFFAFAIXAIIFAAIIFFXXFFA",
        "XFFAXFAFAIFXXAFAAXFFFA",
    ),
    (
        "IIIRRIIRXIIRAIXRXXIIRIAXIXRRFIIAAXIIXRRFFARAXIAFXR",
        "AAFAXRXFIAFFRAXXARXARFRAFXXFFAFARFXFFAFF",
    ),
    (
        "SISRSSSIISISSIXRSSXSSIRSISRASRRSASSXXIXAXIRISSARIA",
        "AXRIXRXAASIASSRXRXSXIRXARAXARIRARAXIXIAIXRXAAA",
    ),
)
STEPS = "IRXAFS"
WORD = 10


def plan_words():
    rows = []
    for pieces in PLAN:
        codes, count, kept = [], 0, False
        for step in "".join(pieces):
            codes.append(STEPS.index(step) + 1)
            if step == "S":
                codes[-1] += kept and count % 3 > 0
                count, kept = count + 1, True
            kept = kept and step != "X"
        rows.append([sum(code << (3 * k) for k, code in enumerate(codes[n:n + WORD])) for n in range(0, len(codes), WORD)])
    longest = max(len(row) for row in rows)
    return [row + [0] * (longest - len(row)) for row in rows]


class Sizes:
    def __init__(self, layers, rows, cols):
        self.layers, self.rows, self.cols = layers, rows, cols
        self.half = layers // 2
        self.tile = rows // 2
        self.units = rows // LANE
        self.sub = self.tile // LANE
        self.full = self.sub * self.tile
        self.pairs = (self.sub + 1) // 2
        self.low = self.sub * (self.sub - 1) // 2
        self.diag = (self.low + self.pairs) * LANE + (self.pairs + 7) // 8 * 8
        self.own = 2 * self.diag + self.full
        self.mid = 4 * self.full
        self.all_units = self.half * self.units
        self.chunks = sum(count for count, _ in SPLIT)
        self.depth = cols // 4 if cols % (4 * LANE) == 0 else cols


def triangles():
    row = lax.broadcasted_iota(jnp.int32, (LANE, LANE), 0)
    col = lax.broadcasted_iota(jnp.int32, (LANE, LANE), 1)
    return row >= col, row == col


def loop(lo, hi, f):
    def body(n, carry):
        f(n)
        return carry

    lax.fori_loop(lo, hi, body, 0)


def exchange_kernel(sz, a, r, lp, rp, psd, psm, rsd, rsm, pc, rb, co, v, acc, stage, cross_stage, ba, bb,
                    load_sem, xs, xr, ls, lr, ds, dr, ss, sr, rss, rsr, cs, cr, fs):
    y = lax.axis_index("kk")
    g = lax.axis_index("g")
    x = g // 2
    c = g % 2
    away = c == x
    home = c != x
    layers, half, units = sz.layers, sz.half, sz.units

    to_x = {"g": (g + 2) % 4}
    to_core = {"g": 2 * x + 1 - c}
    to_y = {"kk": 1 - y}

    def remote(src, dst, send, recv, where):
        return pltpu.make_async_remote_copy(src_ref=src, dst_ref=dst, send_sem=send, recv_sem=recv, device_id=where,
                                            device_id_type=MESH)

    def sized(f):
        def run(q):
            chunk, unit = 0, 0
            for count, size in SPLIT:
                @pl.when((q >= chunk) & (q < chunk + count))
                def _():
                    f(q, unit + (q - chunk) * size, size)

                chunk, unit = chunk + count, unit + count * size

        return run

    def rows_of(ref, u, size, first=0):
        return ref.at[first + u // units, pl.ds(pl.multiple_of(u % units * LANE, LANE), size * LANE)]

    def x_in(q, u, size):
        return remote(rows_of(a, u, size, half * (1 - x)), rows_of(r, u, size), xs.at[q], xr.at[q], to_x)

    def core_in(m):
        return remote(a.at[m], lp.at[m], ls.at[m], lr.at[m], to_core)

    def core_r(q, u, size):
        return remote(rows_of(r, u, size), rows_of(rp, u, size), ds.at[q], dr.at[q], to_core)

    def send_diag(k, m, rows=None):
        src, dst = psd.at[k, m], rsd.at[k, m]
        if rows is not None:
            src, dst = src.at[rows], dst.at[rows]
        return remote(src, dst, ss.at[k, m], sr.at[k, m], to_y)

    def send_mid(m, rows=None):
        src, dst = psm.at[m], rsm.at[m]
        if rows is not None:
            src, dst = src.at[rows], dst.at[rows]
        return remote(src, dst, ss.at[2, m], sr.at[2, m], to_y)

    def send_part(q, u, size):
        return remote(pc.at[pl.ds(u, size), 1 - y], rb.at[pl.ds(u, size)], rss.at[q], rsr.at[q], to_y)

    def send_sum(q, u, size):
        where = {"kk": jnp.where(home, 1 - y, y), "g": jnp.where(home, g, (g + 2) % 4)}
        part = co.at[x, pl.ds(u, size), y]
        return remote(part, part, cs.at[q], cr.at[jnp.where(home, 0, 1), q], where)

    def from_x(q, u, size):
        part = co.at[1 - x, pl.ds(u, size), y]
        return remote(part, part, fs.at[q], cr.at[1, q], to_x)

    def forward(q, u, size):
        part = co.at[1 - x, pl.ds(u, size), y]
        return remote(part, part, fs.at[q], cr.at[2, q], to_y)

    def load(src, dst, k):
        pltpu.make_async_copy(src, dst, load_sem.at[k]).start()

    def loaded(dst, k):
        pltpu.make_async_copy(dst, dst, load_sem.at[k]).wait()

    def store(src, dst):
        copy = pltpu.make_async_copy(src, dst, load_sem.at[4])
        copy.start()
        copy.wait()

    def block(n, rows=sz.rows):
        return v.at[pl.ds(pl.multiple_of(n, LANE), rows)]

    def product(left, right, width):
        acc[:, :width] = jnp.zeros((sz.tile, width), jnp.float32)

        def step(k):
            cols = pl.ds(pl.multiple_of(k * sz.depth, LANE), sz.depth)
            lhs = v[pl.ds(pl.multiple_of(left, LANE), sz.tile), cols]
            rhs = v[pl.ds(pl.multiple_of(right, LANE), width), cols]
            acc[:, :width] += lax.dot_general(lhs, rhs, (((1,), (1,)), ((), ())), preferred_element_type=jnp.float32)

        loop(0, sz.cols // sz.depth, step)

    def put_strips():
        for s in range(sz.sub):
            stage[s * sz.tile:(s + 1) * sz.tile, :] = acc[:, s * LANE:(s + 1) * LANE]

    def put_diag():
        def subtile(i, k):
            return acc[i * LANE:(i + 1) * LANE, k * LANE:(k + 1) * LANE]

        n = 0
        for i in range(sz.sub):
            for k in range(i):
                stage[n:n + LANE, :] = subtile(i, k)
                n += LANE
        lower, equal = triangles()
        tail = (sz.low + sz.pairs) * LANE
        stage[tail:sz.diag, :] = jnp.zeros((sz.diag - tail, LANE), jnp.float32)
        for i in range(0, sz.sub, 2):
            if i + 1 < sz.sub:
                other = subtile(i + 1, i + 1)
                stage[n:n + LANE, :] = jnp.where(lower, subtile(i, i), other)
                stage[tail + i // 2:tail + i // 2 + 1, :] = jnp.sum(jnp.where(equal, other, 0.0), axis=0, keepdims=True)
            else:
                stage[n:n + LANE, :] = subtile(i, i)
            n += LANE

    def same_chip(n, kept):
        m, k = n // 3, n % 3

        def halves(ref, at):
            for d in range(2):
                load(ref.at[m, pl.ds(d * sz.tile, sz.tile)], block(at + d * sz.tile, sz.tile), d)

        @pl.when(k == 0)
        def _():
            halves(a, 0)

        @pl.when((k == 2) & (kept == 0))
        def _():
            halves(lp, sz.rows)

        @pl.when(k == 1)
        def _():
            core_in(m).wait_recv()

            @pl.when(kept == 0)
            def _():
                load(a.at[m], block(0), 2)
                loaded(block(0), 2)

            load(lp.at[m], block(sz.rows), 3)
            loaded(block(sz.rows), 3)

            def middle(i):
                product(i // 2 * sz.tile + (1 - x) * sz.rows, i % 2 * sz.tile + x * sz.rows, sz.tile)
                put_strips()
                rows = pl.ds(pl.multiple_of(i * sz.full, LANE), sz.full)
                store(stage.at[pl.ds(0, sz.full)], psm.at[m, rows])
                send_mid(m, rows).start()

            loop(0, 4, middle)

        @pl.when(k != 1)
        def _():
            which = k // 2
            base = which * sz.rows

            def leave(lo, size):
                rows = pl.ds(pl.multiple_of(lo, 8), size)
                store(stage.at[pl.ds(0, size)], psd.at[which, m, rows])
                send_diag(which, m, rows).start()

            def diagonal(d):
                @pl.when((k == 0) | (kept == 0))
                def _():
                    loaded(block(base + d * sz.tile, sz.tile), d)

                product(base + d * sz.tile, base + d * sz.tile, sz.tile)
                put_diag()
                leave(d * sz.diag, sz.diag)

            loop(0, 2, diagonal)
            product(base + sz.tile, base, sz.tile)
            put_strips()
            leave(2 * sz.diag, sz.full)

    def relay(q, u, size):
        x_in(q, u, size).wait_recv()
        core_r(q, u, size).start()

    def cross(q, u, size):
        j, width = u // units, size * LANE

        @pl.when(x == 0)
        def _():
            @pl.when(home & (u % units == 0))
            def _():
                core_in(j).wait_recv()

            load(a.at[j], block(c * sz.rows), 0)
            load(lp.at[j], block((1 - c) * sz.rows), 1)
            x_in(q, u, size).wait_recv()
            load(rows_of(r, u, size), block(2 * sz.rows, width), 2)
            loaded(block(c * sz.rows), 0)
            loaded(block((1 - c) * sz.rows), 1)
            loaded(block(2 * sz.rows, width), 2)

            def one(n):
                product(n * sz.tile, 2 * sz.rows, width)
                for s in range(size):
                    rows = pl.ds(pl.multiple_of(n % 2 * sz.tile, LANE), sz.tile)
                    cross_stage[s, n // 2, rows, :] = acc[:, s * LANE:(s + 1) * LANE]

            loop(0, 4, one)

        @pl.when(x == 1)
        def _():
            load(a.at[half + j], block(2 * sz.rows), 0)
            load(rows_of(r, u, size), block(c * width, width), 1)
            core_r(q, u, size).wait_recv()
            load(rows_of(rp, u, size), block((1 - c) * width, width), 2)
            loaded(block(2 * sz.rows), 0)
            loaded(block(c * width, width), 1)
            loaded(block((1 - c) * width, width), 2)

            def one(t):
                product(2 * sz.rows + t * sz.tile, 0, 2 * width)
                for i in range(2):
                    for s in range(size):
                        rows = pl.ds(pl.multiple_of(t * sz.tile, LANE), sz.tile)
                        cross_stage[s, i, rows, :] = acc[:, i * width + s * LANE:i * width + (s + 1) * LANE]

            loop(0, 2, one)

        store(cross_stage.at[pl.ds(0, size)], pc.at[pl.ds(u, size)])
        send_part(q, u, size).start()

    def add(q, u, size):
        mine, theirs = ba.at[pl.ds(0, size)], bb.at[pl.ds(0, size)]
        load(pc.at[pl.ds(u, size), y], mine, 0)
        send_part(q, u, size).wait_recv()
        load(rb.at[pl.ds(u, size)], theirs, 1)
        loaded(mine, 0)
        loaded(theirs, 1)
        ba[:size] += bb[:size]
        store(mine, co.at[x, pl.ds(u, size), y])
        send_sum(q, u, size).start()

    def pass_on(q, u, size):
        from_x(q, u, size).wait_recv()
        forward(q, u, size).start()

    barrier = pltpu.get_barrier_semaphore()
    for where in (to_x, to_core, to_y):
        pl.semaphore_signal(barrier, inc=1, device_id=where, device_id_type=MESH)
    pl.semaphore_wait(barrier, 3)

    @pl.when(home)
    def _():
        loop(0, layers, lambda m: core_in(m).start())

    @pl.when(away & (x == 0))
    def _():
        loop(0, half, lambda m: core_in(m).start())

    steps = [sized(lambda *chunk: x_in(*chunk).start()), sized(relay), sized(cross), sized(add), sized(pass_on)]
    words = plan_words()

    def word(n, done):
        code = jnp.int32(0)
        for device, row in enumerate(words):
            for k, value in enumerate(row):
                code = jnp.where((g == device) & (n == k), value, code)

        def digit(_, carry):
            code, done = carry[0], list(carry[1:])
            now = code % 8
            for k, step in enumerate(steps):
                pl.when(now == k + 1)(functools.partial(step, done[k]))
                done[k] += jnp.where(now == k + 1, 1, 0)
            pl.when(now > len(steps))(functools.partial(same_chip, done[-1], now - len(steps) - 1))
            done[-1] += jnp.where(now > len(steps), 1, 0)
            return (code // 8, *done)

        return lax.fori_loop(0, WORD, digit, (code, *done))[1:]

    lax.fori_loop(0, len(words[0]), word, (jnp.int32(0),) * (len(steps) + 1))

    @pl.when(home)
    def _():
        loop(0, layers, lambda m: core_in(m).wait_send())

        def end(*chunk):
            send_sum(*chunk).wait_recv()
            forward(*chunk).wait_recv()
            forward(*chunk).wait_send()

        loop(0, sz.chunks, sized(end))

    @pl.when(away & (x == 0))
    def _():
        loop(0, half, lambda m: core_in(m).wait_send())

    @pl.when(x == 1)
    def _():
        loop(0, sz.chunks, sized(lambda *chunk: core_r(*chunk).wait_send()))

    @pl.when(away)
    def _():
        def end(m):
            for k in range(2):
                send_diag(k, m).wait()
            send_mid(m).wait()

        loop(0, layers, end)

    def sent(*chunk):
        x_in(*chunk).wait_send()
        send_part(*chunk).wait_send()
        send_sum(*chunk).wait_send()

    loop(0, sz.chunks, sized(sent))


def exchange(sz, a):
    f32, bf16 = jnp.float32, jnp.bfloat16
    dma = pltpu.SemaphoreType.DMA
    rows = (sz.rows, sz.cols)
    strip = (sz.rows, LANE)
    most = max(size for _, size in SPLIT)
    outs = [
        ((sz.half,) + rows, bf16),
        ((sz.layers,) + rows, bf16),
        ((sz.half,) + rows, bf16),
        ((2, sz.layers, sz.own, LANE), f32),
        ((sz.layers, sz.mid, LANE), f32),
        ((2, sz.layers, sz.own, LANE), f32),
        ((sz.layers, sz.mid, LANE), f32),
        ((sz.all_units, 2) + strip, f32),
        ((sz.all_units,) + strip, f32),
        ((2, sz.all_units, 2) + strip, f32),
    ]
    n, q = sz.layers, sz.chunks
    res = pl.pallas_call(
        functools.partial(exchange_kernel, sz),
        name="exchange",
        out_shape=[jax.ShapeDtypeStruct(s, d) for s, d in outs],
        in_specs=[pl.BlockSpec(memory_space=pl.ANY)],
        out_specs=[pl.BlockSpec(memory_space=pl.ANY)] * len(outs),
        scratch_shapes=[
            pltpu.VMEM((3 * sz.rows, sz.cols), bf16),
            pltpu.VMEM((sz.tile, sz.tile), f32),
            pltpu.VMEM((sz.full, LANE), f32),
            pltpu.VMEM((most, 2) + strip, f32),
            pltpu.VMEM((most,) + strip, f32),
            pltpu.VMEM((most,) + strip, f32),
            dma((5,)), dma((q,)), dma((q,)), dma((n,)), dma((n,)), dma((q,)), dma((q,)),
            dma((3, n)), dma((3, n)), dma((q,)), dma((q,)), dma((q,)), dma((3, q)), dma((q,)),
        ],
        compiler_params=pltpu.CompilerParams(collective_id=0, has_side_effects=True, vmem_limit_bytes=60 * 2**20),
    )(a)
    return res[3], res[5], res[4], res[6], res[9]


OUTS = 5
INS = 6
DIAGS = 4
ZERO_ROWS = 256


def assemble_kernel(sz, role, psd, rsd, psm, rsm, co, out, ob, ib, db, zeros, out_sem, in_sem, diag_sem, zero_sem):
    t, sub, layers, units = sz.tile, sz.sub, sz.layers, sz.units
    x = role[1]
    lower, equal = triangles()

    def copy(src, dst, sem):
        return pltpu.make_async_copy(src, dst, sem)

    def put(n, i, k, value):
        def at(s):
            return pl.ds(s * LANE if isinstance(s, int) else pl.multiple_of(s * LANE, LANE), LANE)

        ob[n % OUTS, at(i), at(k)] = value

    def free(n):
        @pl.when(n >= OUTS)
        def _():
            copy(ob.at[n % OUTS], out.at[0, 0], out_sem.at[n % OUTS]).wait()

    def leave(n, slot, m):
        copy(ob.at[n % OUTS], out.at[slot, m], out_sem.at[n % OUTS]).start()

    def drain():
        for n in range(OUTS):
            copy(ob.at[n], out.at[0, 0], out_sem.at[n]).wait()

    @pl.when(role[0] == 0)
    def _():
        zeros[...] = jnp.zeros_like(zeros)
        per = sz.rows // ZERO_ROWS

        def zero(n):
            rows = pl.ds(pl.multiple_of(n % per * ZERO_ROWS, ZERO_ROWS), ZERO_ROWS)
            return copy(zeros, out.at[2, n // per, rows], zero_sem)

        def fetch(n):
            m, slot = n // 2, n % 2
            first = m % sz.half * units
            return copy(co.at[m // sz.half, pl.ds(first, units), slot], ib.at[n % INS], in_sem.at[n % INS])

        loop(0, INS, lambda n: fetch(n).start())
        loop(0, layers * per, lambda n: zero(n).start())

        def one(n):
            m, slot = n // 2, n % 2
            fetch(n).wait()
            free(n)

            def unit(u):
                def strip(k):
                    return ib[n % INS, u, k * LANE:(k + 1) * LANE, :]

                @pl.when(m < sz.half)
                def _():
                    for k in range(2 * sub):
                        put(n, u, k, strip(k).T)

                @pl.when(m >= sz.half)
                def _():
                    for k in range(2 * sub):
                        put(n, k, u, strip(k))

            loop(0, units, unit)
            leave(n, slot, m)

            @pl.when(n + INS < 2 * layers)
            def _():
                fetch(n + INS).start()

        loop(0, 2 * layers, one)
        drain()
        loop(0, layers * per, lambda n: zero(n).wait())

    @pl.when(role[0] == 1)
    def _():
        def fetch_diag(n, go):
            for ref, k in ((psd, 0), (rsd, 1)):
                slot = 2 * (n % (DIAGS // 2)) + k
                go(copy(ref.at[n % 2, n // 2], db.at[slot], diag_sem.at[slot]))

        def fetch_mid(m, go):
            for ref, k in ((psm, 0), (rsm, 1)):
                slot = 2 * (m % (INS // 2)) + k
                go(copy(ref.at[m], ib.at[slot], in_sem.at[slot]))

        def start(c):
            c.start()

        def wait(c):
            c.wait()

        def diagonal(n, d):
            fetch_diag(d, wait)
            free(n)
            mine = 2 * (d % (DIAGS // 2))

            def total(row, size=LANE):
                return db[mine, row:row + size, :] + db[mine + 1, row:row + size, :]

            for e in range(2):
                row, first = e * sz.diag, e * sub
                tail = row + (sz.low + sz.pairs) * LANE
                for i in range(sub):
                    for k in range(i):
                        s = total(row)
                        put(n, first + i, first + k, s)
                        put(n, first + k, first + i, s.T)
                        row += LANE
                for i in range(0, sub, 2):
                    s = total(row)
                    flip = s.T
                    put(n, first + i, first + i, jnp.where(lower, s, flip))
                    if i + 1 < sub:
                        line = jnp.broadcast_to(total(tail + i // 2, 1), (LANE, LANE))
                        put(n, first + i + 1, first + i + 1, jnp.where(equal, line, jnp.where(lower, flip, s)))
                    row += LANE
            for k in range(sub):
                for i in range(sub):
                    s = total(2 * sz.diag + k * t + i * LANE)
                    put(n, sub + i, k, s)
                    put(n, k, sub + i, s.T)

        def middle(n, m):
            fetch_mid(m, wait)
            free(n)
            mine = 2 * (m % (INS // 2))

            def strips(u):
                tile, col = u // sub, u % sub
                for i in range(sub):
                    rows = pl.ds(pl.multiple_of(u % 2 * t + i * LANE, LANE), LANE)
                    s = ib[mine, u // 2, rows, :] + ib[mine + 1, u // 2, rows, :]
                    put(n, tile // 2 * sub + i, tile % 2 * sub + col, s)

            loop(0, 4 * sub, strips)

        loop(0, DIAGS // 2, lambda d: fetch_diag(d, start))
        loop(0, INS // 2, lambda m: fetch_mid(m, start))

        def one(m):
            def side(k):
                d = 2 * m + k
                n = 3 * m + k
                diagonal(n, d)
                leave(n, 2 * (x + k - 2 * x * k), m)

                @pl.when(d + DIAGS // 2 < 2 * layers)
                def _():
                    fetch_diag(d + DIAGS // 2, start)

            loop(0, 2, side)
            n = 3 * m + 2
            middle(n, m)
            leave(n, 1, m)

            @pl.when(m + INS // 2 < layers)
            def _():
                fetch_mid(m + INS // 2, start)

        loop(0, layers, one)
        drain()


def assemble(sz, role, psd, rsd, psm, rsm, co):
    f32, dma = jnp.float32, pltpu.SemaphoreType.DMA
    block = (sz.units, sz.rows, LANE)
    hbm = pl.BlockSpec(memory_space=pl.ANY)
    return pl.pallas_call(
        functools.partial(assemble_kernel, sz),
        name="assemble",
        out_shape=jax.ShapeDtypeStruct((3, sz.layers, sz.rows, sz.rows), f32),
        in_specs=[pl.BlockSpec(memory_space=pltpu.SMEM)] + [hbm] * 5,
        out_specs=hbm,
        scratch_shapes=[
            pltpu.VMEM((OUTS, sz.rows, sz.rows), f32),
            pltpu.VMEM((INS,) + block, f32),
            pltpu.VMEM((DIAGS, sz.own, LANE), f32),
            pltpu.VMEM((ZERO_ROWS, sz.rows), f32),
            dma((OUTS,)), dma((INS,)), dma((DIAGS,)), dma,
        ],
        compiler_params=pltpu.CompilerParams(vmem_limit_bytes=60 * 2**20),
    )(role, psd, rsd, psm.reshape((-1,) + block), rsm.reshape((-1,) + block), co)


def solution(mesh):
    def local_part(a_loc):
        sz = Sizes(*a_loc.shape)
        g = lax.axis_index("g")
        x, c = g // 2, g % 2
        role = jnp.stack([jnp.where(c == x, 1, 0), x]).astype(jnp.int32)
        return assemble(sz, role, *exchange(sz, a_loc))[None]

    return jax.shard_map(local_part, mesh=mesh, in_specs=(P(None, ("m", "g"), "kk"),), out_specs=P(("m", "g"), None, None, None, None), check_vma=False)
```

```python
import functools

import jax
import jax.numpy as jnp
from jax import lax
from jax.experimental import pallas as pl
from jax.experimental.pallas import tpu as pltpu
from jax.sharding import PartitionSpec as P


MESH = pl.DeviceIdType.MESH
LANE = 128

SPLIT = ((14, 2), (4, 1))

PLAN = (
    (
        "IIISSISSXIISXASSIIIIIIIIIIIIXASXASSXASXASSXASXSSXA",
        "SXASASXASXASXSASAXXXXSXAAAAA",
    ),
    (
        "IIIIXAIXAIXAIXAIXAIIXXAAIXAIXFFAFIXIFAIXFIFAIIXFAX",
        "FAXFFAXXFAAXFAXFA",
    ),
    (
        "IIIIIIRXIARXARXIARXIARXFIARXIRARXIAXIARXIARXIAIRXI",
        "AIRXARXARXRXAARXARXARFXFFAFFFFFFFFF",
    ),
    (
        "ISSRIIIIISSISRSIXXRSSIXAARSSXARSIXARSXISARSAXRISXS",
        "RASIAXRSSIXRASXARSISXIRASIXARSIXRXRAAAXRAXRAXA",
    ),
)
STEPS = "IRXAFS"
WORD = 10


def plan_words():
    rows = []
    for pieces in PLAN:
        codes, count, kept = [], 0, False
        for step in "".join(pieces):
            codes.append(STEPS.index(step) + 1)
            if step == "S":
                codes[-1] += kept and count % 3 > 0
                count, kept = count + 1, True
            kept = kept and step != "X"
        rows.append([sum(code << (3 * k) for k, code in enumerate(codes[n:n + WORD])) for n in range(0, len(codes), WORD)])
    longest = max(len(row) for row in rows)
    return [row + [0] * (longest - len(row)) for row in rows]


LATE = 3


class Sizes:
    def __init__(self, layers, rows, cols):
        self.layers, self.rows, self.cols = layers, rows, cols
        self.half = layers // 2
        self.tile = rows // 2
        self.units = rows // LANE
        self.sub = self.tile // LANE
        self.full = self.sub * self.tile
        self.pairs = (self.sub + 1) // 2
        self.low = self.sub * (self.sub - 1) // 2
        self.diag = (self.low + self.pairs) * LANE + (self.pairs + 7) // 8 * 8
        self.own = 2 * self.diag + self.full
        self.mid = 4 * self.full
        self.all_units = self.half * self.units
        self.chunks = sum(count for count, _ in SPLIT)
        self.late = LATE
        self.lead = self.units - 2 * LATE
        self.early_units = self.all_units - 2 * LATE
        self.depth = cols // 4 if cols % (4 * LANE) == 0 else cols


def triangles():
    row = lax.broadcasted_iota(jnp.int32, (LANE, LANE), 0)
    col = lax.broadcasted_iota(jnp.int32, (LANE, LANE), 1)
    return row >= col, row == col


def loop(lo, hi, f):
    def body(n, carry):
        f(n)
        return carry

    lax.fori_loop(lo, hi, body, 0)


def exchange_kernel(sz, a, r, lp, rp, psd, psm, rsd, rsm, pc, rb, co, late_diag, late_lo, late_hi, v, acc, stage, cross_stage, ba, bb,
                    load_sem, xs, xr, ls, lr, ds, dr, ss, sr, rss, rsr, cs, cr, fs):
    y = lax.axis_index("kk")
    g = lax.axis_index("g")
    x = g // 2
    c = g % 2
    away = c == x
    home = c != x
    layers, half, units = sz.layers, sz.half, sz.units

    to_x = {"g": (g + 2) % 4}
    to_core = {"g": 2 * x + 1 - c}
    to_y = {"kk": 1 - y}

    def remote(src, dst, send, recv, where):
        return pltpu.make_async_remote_copy(src_ref=src, dst_ref=dst, send_sem=send, recv_sem=recv, device_id=where,
                                            device_id_type=MESH)

    def sized(f):
        def run(q):
            chunk, unit = 0, 0
            for count, size in SPLIT:
                @pl.when((q >= chunk) & (q < chunk + count))
                def _():
                    f(q, unit + (q - chunk) * size, size)

                chunk, unit = chunk + count, unit + count * size

        return run

    def rows_of(ref, u, size, first=0):
        return ref.at[first + u // units, pl.ds(pl.multiple_of(u % units * LANE, LANE), size * LANE)]

    def x_in(q, u, size):
        return remote(rows_of(a, u, size, half * (1 - x)), rows_of(r, u, size), xs.at[q], xr.at[q], to_x)

    def core_in(m):
        return remote(a.at[m], lp.at[m], ls.at[m], lr.at[m], to_core)

    def core_r(q, u, size):
        return remote(rows_of(r, u, size), rows_of(rp, u, size), ds.at[q], dr.at[q], to_core)

    def send_diag(k, m, rows=None):
        src, dst = psd.at[k, m], rsd.at[k, m]
        if rows is not None:
            src, dst = src.at[rows], dst.at[rows]
        return remote(src, dst, ss.at[k, m], sr.at[k, m], to_y)

    def send_mid(m, rows=None):
        src, dst = psm.at[m], rsm.at[m]
        if rows is not None:
            src, dst = src.at[rows], dst.at[rows]
        return remote(src, dst, ss.at[2, m], sr.at[2, m], to_y)

    def send_part(q, u, size):
        return remote(pc.at[pl.ds(u, size), 1 - y], rb.at[pl.ds(u, size)], rss.at[q], rsr.at[q], to_y)

    def send_sum(q, u, size):
        where = {"kk": jnp.where(home, 1 - y, y), "g": jnp.where(home, g, (g + 2) % 4)}
        part = co.at[x, pl.ds(u, size), y]
        return remote(part, part, cs.at[q], cr.at[jnp.where(home, 0, 1), q], where)

    def from_x(q, u, size):
        part = co.at[1 - x, pl.ds(u, size), y]
        return remote(part, part, fs.at[q], cr.at[1, q], to_x)

    def forward(q, u, size):
        part = co.at[1 - x, pl.ds(u, size), y]
        return remote(part, part, fs.at[q], cr.at[2, q], to_y)

    def load(src, dst, k):
        pltpu.make_async_copy(src, dst, load_sem.at[k]).start()

    def loaded(dst, k):
        pltpu.make_async_copy(dst, dst, load_sem.at[k]).wait()

    def store(src, dst):
        copy = pltpu.make_async_copy(src, dst, load_sem.at[4])
        copy.start()
        copy.wait()

    def block(n, rows=sz.rows):
        return v.at[pl.ds(pl.multiple_of(n, LANE), rows)]

    def product(left, right, width):
        acc[:, :width] = jnp.zeros((sz.tile, width), jnp.float32)

        def step(k):
            cols = pl.ds(pl.multiple_of(k * sz.depth, LANE), sz.depth)
            lhs = v[pl.ds(pl.multiple_of(left, LANE), sz.tile), cols]
            rhs = v[pl.ds(pl.multiple_of(right, LANE), width), cols]
            acc[:, :width] += lax.dot_general(lhs, rhs, (((1,), (1,)), ((), ())), preferred_element_type=jnp.float32)

        loop(0, sz.cols // sz.depth, step)

    def put_strips():
        for s in range(sz.sub):
            stage[s * sz.tile:(s + 1) * sz.tile, :] = acc[:, s * LANE:(s + 1) * LANE]

    def put_diag():
        def subtile(i, k):
            return acc[i * LANE:(i + 1) * LANE, k * LANE:(k + 1) * LANE]

        n = 0
        for i in range(sz.sub):
            for k in range(i):
                stage[n:n + LANE, :] = subtile(i, k)
                n += LANE
        lower, equal = triangles()
        tail = (sz.low + sz.pairs) * LANE
        stage[tail:sz.diag, :] = jnp.zeros((sz.diag - tail, LANE), jnp.float32)
        for i in range(0, sz.sub, 2):
            if i + 1 < sz.sub:
                other = subtile(i + 1, i + 1)
                stage[n:n + LANE, :] = jnp.where(lower, subtile(i, i), other)
                stage[tail + i // 2:tail + i // 2 + 1, :] = jnp.sum(jnp.where(equal, other, 0.0), axis=0, keepdims=True)
            else:
                stage[n:n + LANE, :] = subtile(i, i)
            n += LANE

    def same_chip(n, kept):
        m, k = n // 3, n % 3

        def halves(ref, at):
            for d in range(2):
                load(ref.at[m, pl.ds(d * sz.tile, sz.tile)], block(at + d * sz.tile, sz.tile), d)

        @pl.when(k == 0)
        def _():
            halves(a, 0)

        @pl.when((k == 2) & (kept == 0))
        def _():
            halves(lp, sz.rows)

        @pl.when(k == 1)
        def _():
            core_in(m).wait_recv()

            @pl.when(kept == 0)
            def _():
                load(a.at[m], block(0), 2)
                loaded(block(0), 2)

            load(lp.at[m], block(sz.rows), 3)
            loaded(block(sz.rows), 3)

            def middle(i):
                product(i // 2 * sz.tile + (1 - x) * sz.rows, i % 2 * sz.tile + x * sz.rows, sz.tile)
                put_strips()
                rows = pl.ds(pl.multiple_of(i * sz.full, LANE), sz.full)
                store(stage.at[pl.ds(0, sz.full)], psm.at[m, rows])
                send_mid(m, rows).start()

            loop(0, 4, middle)

        @pl.when(k != 1)
        def _():
            which = k // 2
            base = which * sz.rows

            def leave(lo, size):
                rows = pl.ds(pl.multiple_of(lo, 8), size)

                @pl.when(n == 3 * layers - 1)
                def _():
                    store(stage.at[pl.ds(0, size)], late_diag.at[rows])

                @pl.when(n < 3 * layers - 1)
                def _():
                    store(stage.at[pl.ds(0, size)], psd.at[which, m, rows])
                    send_diag(which, m, rows).start()

            def diagonal(d):
                @pl.when((k == 0) | (kept == 0))
                def _():
                    loaded(block(base + d * sz.tile, sz.tile), d)

                product(base + d * sz.tile, base + d * sz.tile, sz.tile)
                put_diag()
                leave(d * sz.diag, sz.diag)

            loop(0, 2, diagonal)
            product(base + sz.tile, base, sz.tile)
            put_strips()
            leave(2 * sz.diag, sz.full)

    def relay(q, u, size):
        x_in(q, u, size).wait_recv()
        core_r(q, u, size).start()

    def cross(q, u, size):
        j, width = u // units, size * LANE

        @pl.when(x == 0)
        def _():
            @pl.when(home & (u % units == 0))
            def _():
                core_in(j).wait_recv()

            load(a.at[j], block(c * sz.rows), 0)
            load(lp.at[j], block((1 - c) * sz.rows), 1)
            x_in(q, u, size).wait_recv()
            load(rows_of(r, u, size), block(2 * sz.rows, width), 2)
            loaded(block(c * sz.rows), 0)
            loaded(block((1 - c) * sz.rows), 1)
            loaded(block(2 * sz.rows, width), 2)

            def one(n):
                product(n * sz.tile, 2 * sz.rows, width)
                for s in range(size):
                    rows = pl.ds(pl.multiple_of(n % 2 * sz.tile, LANE), sz.tile)
                    cross_stage[s, n // 2, rows, :] = acc[:, s * LANE:(s + 1) * LANE]

            loop(0, 4, one)

        @pl.when(x == 1)
        def _():
            load(a.at[half + j], block(2 * sz.rows), 0)
            load(rows_of(r, u, size), block(c * width, width), 1)
            core_r(q, u, size).wait_recv()
            load(rows_of(rp, u, size), block((1 - c) * width, width), 2)
            loaded(block(2 * sz.rows), 0)
            loaded(block(c * width, width), 1)
            loaded(block((1 - c) * width, width), 2)

            def one(t):
                product(2 * sz.rows + t * sz.tile, 0, 2 * width)
                for i in range(2):
                    for s in range(size):
                        rows = pl.ds(pl.multiple_of(t * sz.tile, LANE), sz.tile)
                        cross_stage[s, i, rows, :] = acc[:, i * width + s * LANE:i * width + (s + 1) * LANE]

            loop(0, 2, one)

        store(cross_stage.at[pl.ds(0, size)], pc.at[pl.ds(u, size)])
        send_part(q, u, size).start()

    def add(q, u, size):
        mine, theirs = ba.at[pl.ds(0, size)], bb.at[pl.ds(0, size)]
        load(pc.at[pl.ds(u, size), y], mine, 0)
        send_part(q, u, size).wait_recv()
        load(rb.at[pl.ds(u, size)], theirs, 1)
        loaded(mine, 0)
        loaded(theirs, 1)
        ba[:size] += bb[:size]
        over = u - sz.early_units

        @pl.when(home | (over < 0))
        def _():
            store(mine, co.at[x, pl.ds(u, size), y])
            send_sum(q, u, size).start()

        @pl.when(away & (over >= 0) & (over < sz.late))
        def _():
            store(mine, late_lo.at[pl.ds(over, size)])

        @pl.when(away & (over >= sz.late))
        def _():
            store(mine, late_hi.at[pl.ds(over - sz.late, size)])

    def pass_on(q, u, size):
        from_x(q, u, size).wait_recv()
        forward(q, u, size).start()

    barrier = pltpu.get_barrier_semaphore()
    for where in (to_x, to_core, to_y):
        pl.semaphore_signal(barrier, inc=1, device_id=where, device_id_type=MESH)
    pl.semaphore_wait(barrier, 3)

    @pl.when(home)
    def _():
        loop(0, layers, lambda m: core_in(m).start())

    @pl.when(away & (x == 0))
    def _():
        loop(0, half, lambda m: core_in(m).start())

    steps = [sized(lambda *chunk: x_in(*chunk).start()), sized(relay), sized(cross), sized(add), sized(pass_on)]
    words = plan_words()

    def word(n, done):
        code = jnp.int32(0)
        for device, row in enumerate(words):
            for k, value in enumerate(row):
                code = jnp.where((g == device) & (n == k), value, code)

        def digit(_, carry):
            code, done = carry[0], list(carry[1:])
            now = code % 8
            for k, step in enumerate(steps):
                pl.when(now == k + 1)(functools.partial(step, done[k]))
                done[k] += jnp.where(now == k + 1, 1, 0)
            pl.when(now > len(steps))(functools.partial(same_chip, done[-1], now - len(steps) - 1))
            done[-1] += jnp.where(now > len(steps), 1, 0)
            return (code // 8, *done)

        return lax.fori_loop(0, WORD, digit, (code, *done))[1:]

    lax.fori_loop(0, len(words[0]), word, (jnp.int32(0),) * (len(steps) + 1))

    @pl.when(home)
    def _():
        loop(0, layers, lambda m: core_in(m).wait_send())

        def end(q, u, size):
            send_sum(q, u, size).wait_recv()

            @pl.when(u < sz.early_units)
            def _():
                forward(q, u, size).wait_recv()
                forward(q, u, size).wait_send()

        loop(0, sz.chunks, sized(end))

    @pl.when(away & (x == 0))
    def _():
        loop(0, half, lambda m: core_in(m).wait_send())

    @pl.when(x == 1)
    def _():
        loop(0, sz.chunks, sized(lambda *chunk: core_r(*chunk).wait_send()))

    @pl.when(away)
    def _():
        def end(m):
            send_diag(0, m).wait()
            send_mid(m).wait()

            @pl.when(m < layers - 1)
            def _():
                send_diag(1, m).wait()

        loop(0, layers, end)

    def sent(q, u, size):
        x_in(q, u, size).wait_send()
        send_part(q, u, size).wait_send()

        @pl.when(home | (u < sz.early_units))
        def _():
            send_sum(q, u, size).wait_send()

    loop(0, sz.chunks, sized(sent))


def exchange(sz, a):
    f32, bf16 = jnp.float32, jnp.bfloat16
    dma = pltpu.SemaphoreType.DMA
    rows = (sz.rows, sz.cols)
    strip = (sz.rows, LANE)
    most = max(size for _, size in SPLIT)
    outs = [
        ((sz.half,) + rows, bf16),
        ((sz.layers,) + rows, bf16),
        ((sz.half,) + rows, bf16),
        ((2, sz.layers, sz.own, LANE), f32),
        ((sz.layers, sz.mid, LANE), f32),
        ((2, sz.layers, sz.own, LANE), f32),
        ((sz.layers, sz.mid, LANE), f32),
        ((sz.all_units, 2) + strip, f32),
        ((sz.all_units,) + strip, f32),
        ((2, sz.all_units, 2) + strip, f32),
        ((sz.own, LANE), f32),
        ((sz.late,) + strip, f32),
        ((sz.late,) + strip, f32),
    ]
    n, q = sz.layers, sz.chunks
    res = pl.pallas_call(
        functools.partial(exchange_kernel, sz),
        name="exchange",
        out_shape=[jax.ShapeDtypeStruct(s, d) for s, d in outs],
        in_specs=[pl.BlockSpec(memory_space=pl.ANY)],
        out_specs=[pl.BlockSpec(memory_space=pl.ANY)] * len(outs),
        scratch_shapes=[
            pltpu.VMEM((3 * sz.rows, sz.cols), bf16),
            pltpu.VMEM((sz.tile, sz.tile), f32),
            pltpu.VMEM((sz.full, LANE), f32),
            pltpu.VMEM((most, 2) + strip, f32),
            pltpu.VMEM((most,) + strip, f32),
            pltpu.VMEM((most,) + strip, f32),
            dma((5,)), dma((q,)), dma((q,)), dma((n,)), dma((n,)), dma((q,)), dma((q,)),
            dma((3, n)), dma((3, n)), dma((q,)), dma((q,)), dma((q,)), dma((3, q)), dma((q,)),
        ],
        compiler_params=pltpu.CompilerParams(collective_id=0, has_side_effects=True, vmem_limit_bytes=60 * 2**20),
    )(a)
    return (res[3], res[5], res[4], res[6], res[9]), res[10:]


OUTS = 5
INS = 6
DIAGS = 4
ZERO_ROWS = 256
HOME_PARTS = (0, 4, 9, 14)
AWAY_PARTS = (0, 3, 6, 8)


class Blocks:
    def __init__(self, sz, out, ob, out_sem):
        self.sz, self.out, self.ob, self.out_sem = sz, out, ob, out_sem
        self.lower, self.equal = triangles()

    def put(self, b, i, k, value):
        def at(n):
            return pl.ds(n * LANE if isinstance(n, int) else pl.multiple_of(n * LANE, LANE), LANE)

        self.ob[b, at(i), at(k)] = value

    def free(self, n):
        @pl.when(n >= OUTS)
        def _():
            self.done(n % OUTS)

    def leave(self, n, slot, m):
        b = n % OUTS
        pltpu.make_async_copy(self.ob.at[b], self.out.at[slot, m], self.out_sem.at[b]).start()

    def done(self, b):
        pltpu.make_async_copy(self.ob.at[b], self.out.at[0, 0], self.out_sem.at[b]).wait()

    def drain(self, count):
        for b in range(min(OUTS, count)):
            self.done(b)

    def unit(self, b, u, strip, transposed):
        count = 2 * self.sz.sub

        @pl.when(transposed)
        def _():
            for k in range(count):
                self.put(b, u, k, strip(k).T)

        @pl.when(jnp.logical_not(transposed))
        def _():
            for k in range(count):
                self.put(b, k, u, strip(k))

    def diagonal(self, b, total):
        sz, sub = self.sz, self.sz.sub
        for e in range(2):
            row, first = e * sz.diag, e * sub
            tail = row + (sz.low + sz.pairs) * LANE
            for i in range(sub):
                for k in range(i):
                    s = total(row, LANE)
                    self.put(b, first + i, first + k, s)
                    self.put(b, first + k, first + i, s.T)
                    row += LANE
            for i in range(0, sub, 2):
                s = total(row, LANE)
                flip = s.T
                self.put(b, first + i, first + i, jnp.where(self.lower, s, flip))
                if i + 1 < sub:
                    line = jnp.broadcast_to(total(tail + i // 2, 1), (LANE, LANE))
                    other = jnp.where(self.equal, line, jnp.where(self.lower, flip, s))
                    self.put(b, first + i + 1, first + i + 1, other)
                row += LANE
        for k in range(sub):
            for i in range(sub):
                s = total(2 * sz.diag + k * sz.tile + i * LANE, LANE)
                self.put(b, sub + i, k, s)
                self.put(b, k, sub + i, s.T)


def assemble_kernel(sz, number, *refs):
    first, late_mine, late_theirs = number == 0, None, None
    role, psd, rsd, psm, rsm, co = refs[:6]
    if AWAY_PARTS[number + 1] == sz.layers:
        late_mine, late_theirs = refs[6:8]
    out = refs[-9]
    ob, ib, db, zeros, out_sem, in_sem, diag_sem, zero_sem = refs[-8:]
    layers, half, units, sub, t = sz.layers, sz.half, sz.units, sz.sub, sz.tile
    x = role[1]
    blocks = Blocks(sz, out, ob, out_sem)

    @pl.when(role[0] == 0)
    def _():
        lo, hi = HOME_PARTS[number:number + 2]
        per = sz.rows // ZERO_ROWS

        def zero(n):
            rows = pl.ds(pl.multiple_of(n % per * ZERO_ROWS, ZERO_ROWS), ZERO_ROWS)
            return pltpu.make_async_copy(zeros, out.at[2, n // per, rows], zero_sem)

        def place(n):
            over = jnp.where(n >= layers, 1, 0)
            return x + over - 2 * x * over, n // 2 - over * half, n % 2

        def fetch(n):
            side, j, slot = place(n)
            b = (n - lo) % INS
            return pltpu.make_async_copy(co.at[side, pl.ds(j * units, units), slot], ib.at[b], in_sem.at[b])

        loop(lo, min(lo + INS, hi), lambda n: fetch(n).start())
        if first:
            zeros[...] = jnp.zeros_like(zeros)
            loop(0, layers * per, lambda n: zero(n).start())

        def one(n):
            side, j, slot = place(n)
            k = n - lo
            fetch(n).wait()
            blocks.free(k)

            def unit(u):
                blocks.unit(k % OUTS, u, lambda i: ib[k % INS, u, i * LANE:(i + 1) * LANE, :], side == 0)

            loop(0, units, unit)
            blocks.leave(k, slot, side * half + j)

            @pl.when(n + INS < hi)
            def _():
                fetch(n + INS).start()

        loop(lo, hi, one)
        blocks.drain(hi - lo)
        if first:
            loop(0, layers * per, lambda n: zero(n).wait())

    @pl.when(role[0] == 1)
    def _():
        lo, hi = AWAY_PARTS[number:number + 2]
        depth, diag_depth = INS // 2, DIAGS // 2

        def fetch_diag(d, go):
            for ref, late, k in ((psd, late_mine, 0), (rsd, late_theirs, 1)):
                b = 2 * ((d - 2 * lo) % diag_depth) + k
                if late is None:
                    go(pltpu.make_async_copy(ref.at[d % 2, d // 2], db.at[b], diag_sem.at[b]))
                else:
                    @pl.when(d == 2 * layers - 1)
                    def _():
                        go(pltpu.make_async_copy(late, db.at[b], diag_sem.at[b]))

                    @pl.when(d < 2 * layers - 1)
                    def _():
                        go(pltpu.make_async_copy(ref.at[d % 2, d // 2], db.at[b], diag_sem.at[b]))

        def fetch_mid(m, go):
            for ref, k in ((psm, 0), (rsm, 1)):
                b = 2 * ((m - lo) % depth) + k
                go(pltpu.make_async_copy(ref.at[m], ib.at[b], in_sem.at[b]))

        def start(c):
            c.start()

        def wait(c):
            c.wait()

        loop(2 * lo, 2 * lo + diag_depth, lambda d: fetch_diag(d, start))
        loop(lo, min(lo + depth, hi), lambda m: fetch_mid(m, start))

        def one(m):
            def side(k):
                d, n = 2 * m + k, 3 * (m - lo) + k
                mine = 2 * ((d - 2 * lo) % diag_depth)
                fetch_diag(d, wait)
                blocks.free(n)
                blocks.diagonal(n % OUTS, lambda row, size: db[mine, row:row + size, :] + db[mine + 1, row:row + size, :])
                blocks.leave(n, 2 * (x + k - 2 * x * k), m)

                @pl.when(d + diag_depth < 2 * hi)
                def _():
                    fetch_diag(d + diag_depth, start)

            loop(0, 2, side)
            n = 3 * (m - lo) + 2
            mine = 2 * ((m - lo) % depth)
            fetch_mid(m, wait)
            blocks.free(n)

            def strips(u):
                tile, col = u // sub, u % sub
                for i in range(sub):
                    rows = pl.ds(pl.multiple_of(u % 2 * t + i * LANE, LANE), LANE)
                    s = ib[mine, u // 2, rows, :] + ib[mine + 1, u // 2, rows, :]
                    blocks.put(n % OUTS, tile // 2 * sub + i, tile % 2 * sub + col, s)

            loop(0, 4 * sub, strips)
            blocks.leave(n, 1, m)

            @pl.when(m + depth < hi)
            def _():
                fetch_mid(m + depth, start)

        loop(lo, hi, one)
        blocks.drain(3 * (hi - lo))


def assemble(sz, number, role, parts, late=(), out=None):
    f32, dma = jnp.float32, pltpu.SemaphoreType.DMA
    block = (sz.units, sz.rows, LANE)
    hbm = pl.BlockSpec(memory_space=pl.ANY)
    psd, rsd, psm, rsm, co = parts
    args = [role, psd, rsd, psm.reshape((-1,) + block), rsm.reshape((-1,) + block), co, *late]
    if out is not None:
        args.append(out)
    moved = sz.layers * sz.rows * sz.rows * 4 * 2
    return pl.pallas_call(
        functools.partial(assemble_kernel, sz, number),
        out_shape=jax.ShapeDtypeStruct((3, sz.layers, sz.rows, sz.rows), f32),
        in_specs=[pl.BlockSpec(memory_space=pltpu.SMEM)] + [hbm] * (len(args) - 1),
        out_specs=hbm,
        scratch_shapes=[
            pltpu.VMEM((OUTS, sz.rows, sz.rows), f32),
            pltpu.VMEM((INS,) + block, f32),
            pltpu.VMEM((DIAGS, sz.own, LANE), f32),
            pltpu.VMEM((ZERO_ROWS, sz.rows), f32),
            dma((OUTS,)), dma((INS,)), dma((DIAGS,)), dma,
        ],
        input_output_aliases={} if out is None else {len(args) - 1: 0},
        cost_estimate=pl.CostEstimate(flops=10**10, bytes_accessed=moved, transcendentals=0),
        compiler_params=pltpu.CompilerParams(vmem_limit_bytes=60 * 2**20),
    )(*args)


def finish_kernel(sz, last, role, *refs):
    count = 1 if last else 3
    pieces, co, out = refs[:count], refs[count], refs[count + 2]
    ob, ib, hb, out_sem, in_sem, head_sem = refs[-6:]
    side = 1 - role[1]
    m = side * sz.half + sz.half - 1
    slots = role[2], 1 - role[2]
    tail = sz.lead + sz.late
    blocks = Blocks(sz, out, ob, out_sem)

    @pl.when(role[0] == 0)
    def _():
        def heads(b):
            first = (sz.half - 1) * sz.units
            return pltpu.make_async_copy(co.at[side, pl.ds(first, sz.lead), slots[b]], hb.at[b], head_sem.at[b])

        copies = [pltpu.make_async_copy(ref, ib.at[n], in_sem.at[n]) for n, ref in enumerate(pieces)]
        for c in copies:
            c.start()

        def head(b):
            heads(b).wait()
            loop(0, sz.lead, lambda u: blocks.unit(b, u, lambda k: hb[b, u, k * LANE:(k + 1) * LANE, :], side == 0))

        def units(n, b, first):
            copies[n].wait()
            loop(0, sz.late, lambda u: blocks.unit(b, first + u, lambda k: ib[n, u, k * LANE:(k + 1) * LANE, :], side == 0))

        def part(b, first, size, go):
            rows = pl.ds(first * LANE, size * LANE)

            @pl.when(side == 0)
            def _():
                go(pltpu.make_async_copy(ob.at[b, rows], out.at[slots[b], m, rows], out_sem.at[b]))

            @pl.when(side == 1)
            def _():
                go(pltpu.make_async_copy(ob.at[b, :, rows], out.at[slots[b], m, :, rows], out_sem.at[b]))

        def start(c):
            c.start()

        def wait(c):
            c.wait()

        if last:
            units(0, 1, tail)
            part(1, tail, sz.late, start)
            part(1, tail, sz.late, wait)
        else:
            heads(0).start()
            heads(1).start()
            head(0)
            units(0, 0, sz.lead)
            units(1, 0, tail)
            blocks.leave(0, slots[0], m)
            head(1)
            units(2, 1, sz.lead)
            part(1, 0, tail, start)
            blocks.done(0)
            part(1, 0, tail, wait)


def finish(sz, last, role, pieces, co, out):
    f32, dma = jnp.float32, pltpu.SemaphoreType.DMA
    count = len(pieces)
    hbm = pl.BlockSpec(memory_space=pl.ANY)
    return pl.pallas_call(
        functools.partial(finish_kernel, sz, last),
        name="finish_last" if last else "finish",
        out_shape=jax.ShapeDtypeStruct(out.shape, f32),
        in_specs=[pl.BlockSpec(memory_space=pltpu.SMEM)] + [hbm] * (count + 2),
        out_specs=hbm,
        scratch_shapes=[
            pltpu.VMEM((2, sz.rows, sz.rows), f32),
            pltpu.VMEM((count, sz.late, sz.rows, LANE), f32),
            pltpu.VMEM((2, sz.lead, sz.rows, LANE), f32),
            dma((2,)), dma((count,)), dma((2,)),
        ],
        input_output_aliases={count + 2: 0},
        cost_estimate=pl.CostEstimate(flops=3 * 10**9, bytes_accessed=8 * sz.rows * sz.rows, transcendentals=0),
        compiler_params=pltpu.CompilerParams(vmem_limit_bytes=32 * 2**20),
    )(role, *pieces, co, out)


def solution(mesh):
    width = mesh.shape["g"]
    axes = ("kk", "g")

    def pairs(moves):
        return [(a * width + b, c * width + d) for (a, b), (c, d) in moves]

    ys = range(mesh.shape["kk"])
    over_x = pairs([((y, g), (y, (g + 2) % 4)) for y in ys for g in (0, 3)])
    away_y = pairs([((y, g), (1 - y, g)) for y in ys for g in (0, 3)])
    home_y = pairs([((y, g), (1 - y, g)) for y in ys for g in (1, 2)])

    def local_part(a_loc):
        sz = Sizes(*a_loc.shape)
        g = lax.axis_index("g")
        x, c = g // 2, g % 2
        role = jnp.stack([jnp.where(c == x, 1, 0), x, lax.axis_index("kk")]).astype(jnp.int32)
        parts, (late_diag, late_lo, late_hi) = exchange(sz, a_loc)
        lo = lax.ppermute(late_lo, axes, over_x)
        hi = lax.ppermute(late_hi, axes, over_x)
        theirs = lax.ppermute(late_diag, axes, away_y)
        lo_too = lax.ppermute(lo, axes, home_y)
        hi_too = lax.ppermute(hi, axes, home_y)
        out = assemble(sz, 0, role, parts)
        out = assemble(sz, 1, role, parts, (), out)
        out = assemble(sz, 2, role, parts, (late_diag, theirs), out)
        out = finish(sz, False, role, (lo, hi, lo_too), parts[-1], out)
        out = finish(sz, True, role, (hi_too,), parts[-1], out)
        return out[None]

    return jax.shard_map(local_part, mesh=mesh, in_specs=(P(None, ("m", "g"), "kk"),), out_specs=P(("m", "g"), None, None, None, None), check_vma=False)
```

```python
import functools

import jax
import jax.numpy as jnp
from jax import lax
from jax.experimental import pallas as pl
from jax.experimental.pallas import tpu as pltpu
from jax.sharding import PartitionSpec as P


MESH = pl.DeviceIdType.MESH
LANE = 128

SPLIT = ((14, 2), (4, 1))

PLAN = (
    (
        "IIISSISSXIISXASSIIIIIIIIIIIIXASXASSXASXASSXASXSSXA",
        "SXASASXASXASXSASAXXXXSXAAAAA",
    ),
    (
        "IIIIXAIXAIXAIXAIXAIIXXAAIXAIXFFAFIXIFAIXFIFAIIXFAX",
        "FAXFFAXXFAAXFAXFA",
    ),
    (
        "IIIIIIRXIARXARXIARXIARXFIARXIRARXIAXIARXIARXIAIRXI",
        "AIRXARXARXRXAARXARXARFXFFAFFFFFFFFF",
    ),
    (
        "ISSRIIIIISSISRSIXXRSSIXAARSSXARSIXARSXISARSAXRISXS",
        "RASIAXRSSIXRASXARSISXIRASIXARSIXRXRAAAXRAXRAXA",
    ),
)
STEPS = "IRXAFS"
WORD = 10


def plan_words():
    rows = []
    for pieces in PLAN:
        codes, count, kept = [], 0, False
        for step in "".join(pieces):
            codes.append(STEPS.index(step) + 1)
            if step == "S":
                codes[-1] += kept and count % 3 > 0
                count, kept = count + 1, True
            kept = kept and step != "X"
        rows.append([sum(code << (3 * k) for k, code in enumerate(codes[n:n + WORD])) for n in range(0, len(codes), WORD)])
    longest = max(len(row) for row in rows)
    return [row + [0] * (longest - len(row)) for row in rows]


LATE = 3


class Sizes:
    def __init__(self, layers, rows, cols):
        self.layers, self.rows, self.cols = layers, rows, cols
        self.half = layers // 2
        self.tile = rows // 2
        self.units = rows // LANE
        self.sub = self.tile // LANE
        self.full = self.sub * self.tile
        self.pairs = (self.sub + 1) // 2
        self.low = self.sub * (self.sub - 1) // 2
        self.diag = (self.low + self.pairs) * LANE + (self.pairs + 7) // 8 * 8
        self.own = 2 * self.diag + self.full
        self.mid = 4 * self.full
        self.all_units = self.half * self.units
        self.chunks = sum(count for count, _ in SPLIT)
        self.late = LATE
        self.lead = self.units - 2 * LATE
        self.early_units = self.all_units - 2 * LATE
        self.depth = cols // 4 if cols % (4 * LANE) == 0 else cols


def triangles():
    row = lax.broadcasted_iota(jnp.int32, (LANE, LANE), 0)
    col = lax.broadcasted_iota(jnp.int32, (LANE, LANE), 1)
    return row >= col, row == col


def loop(lo, hi, f):
    def body(n, carry):
        f(n)
        return carry

    lax.fori_loop(lo, hi, body, 0)


def exchange_kernel(sz, a, r, lp, rp, psd, psm, rsd, rsm, pc, rb, co, late_diag, late_lo, late_hi, v, acc, stage, cross_stage, ba, bb,
                    load_sem, xs, xr, ls, lr, ds, dr, ss, sr, rss, rsr, cs, cr, fs):
    y = lax.axis_index("kk")
    g = lax.axis_index("g")
    x = g // 2
    c = g % 2
    away = c == x
    home = c != x
    layers, half, units = sz.layers, sz.half, sz.units

    to_x = {"g": (g + 2) % 4}
    to_core = {"g": 2 * x + 1 - c}
    to_y = {"kk": 1 - y}

    def remote(src, dst, send, recv, where):
        return pltpu.make_async_remote_copy(src_ref=src, dst_ref=dst, send_sem=send, recv_sem=recv, device_id=where,
                                            device_id_type=MESH)

    def sized(f):
        def run(q):
            chunk, unit = 0, 0
            for count, size in SPLIT:
                @pl.when((q >= chunk) & (q < chunk + count))
                def _():
                    f(q, unit + (q - chunk) * size, size)

                chunk, unit = chunk + count, unit + count * size

        return run

    def rows_of(ref, u, size, first=0):
        return ref.at[first + u // units, pl.ds(pl.multiple_of(u % units * LANE, LANE), size * LANE)]

    def x_in(q, u, size):
        return remote(rows_of(a, u, size, half * (1 - x)), rows_of(r, u, size), xs.at[q], xr.at[q], to_x)

    def core_in(m):
        return remote(a.at[m], lp.at[m], ls.at[m], lr.at[m], to_core)

    def core_r(q, u, size):
        return remote(rows_of(r, u, size), rows_of(rp, u, size), ds.at[q], dr.at[q], to_core)

    def send_diag(k, m, rows=None):
        src, dst = psd.at[k, m], rsd.at[k, m]
        if rows is not None:
            src, dst = src.at[rows], dst.at[rows]
        return remote(src, dst, ss.at[k, m], sr.at[k, m], to_y)

    def send_mid(m, rows=None):
        src, dst = psm.at[m], rsm.at[m]
        if rows is not None:
            src, dst = src.at[rows], dst.at[rows]
        return remote(src, dst, ss.at[2, m], sr.at[2, m], to_y)

    def send_part(q, u, size):
        return remote(pc.at[pl.ds(u, size), 1 - y], rb.at[pl.ds(u, size)], rss.at[q], rsr.at[q], to_y)

    def send_sum(q, u, size):
        where = {"kk": jnp.where(home, 1 - y, y), "g": jnp.where(home, g, (g + 2) % 4)}
        part = co.at[x, pl.ds(u, size), y]
        return remote(part, part, cs.at[q], cr.at[jnp.where(home, 0, 1), q], where)

    def from_x(q, u, size):
        part = co.at[1 - x, pl.ds(u, size), y]
        return remote(part, part, fs.at[q], cr.at[1, q], to_x)

    def forward(q, u, size):
        part = co.at[1 - x, pl.ds(u, size), y]
        return remote(part, part, fs.at[q], cr.at[2, q], to_y)

    def load(src, dst, k):
        pltpu.make_async_copy(src, dst, load_sem.at[k]).start()

    def loaded(dst, k):
        pltpu.make_async_copy(dst, dst, load_sem.at[k]).wait()

    def store(src, dst):
        copy = pltpu.make_async_copy(src, dst, load_sem.at[4])
        copy.start()
        copy.wait()

    def block(n, rows=sz.rows):
        return v.at[pl.ds(pl.multiple_of(n, LANE), rows)]

    def product(left, right, width):
        acc[:, :width] = jnp.zeros((sz.tile, width), jnp.float32)

        def step(k):
            cols = pl.ds(pl.multiple_of(k * sz.depth, LANE), sz.depth)
            lhs = v[pl.ds(pl.multiple_of(left, LANE), sz.tile), cols]
            rhs = v[pl.ds(pl.multiple_of(right, LANE), width), cols]
            acc[:, :width] += lax.dot_general(lhs, rhs, (((1,), (1,)), ((), ())), preferred_element_type=jnp.float32)

        loop(0, sz.cols // sz.depth, step)

    def put_strips():
        for s in range(sz.sub):
            stage[s * sz.tile:(s + 1) * sz.tile, :] = acc[:, s * LANE:(s + 1) * LANE]

    def put_diag():
        def subtile(i, k):
            return acc[i * LANE:(i + 1) * LANE, k * LANE:(k + 1) * LANE]

        n = 0
        for i in range(sz.sub):
            for k in range(i):
                stage[n:n + LANE, :] = subtile(i, k)
                n += LANE
        lower, equal = triangles()
        tail = (sz.low + sz.pairs) * LANE
        stage[tail:sz.diag, :] = jnp.zeros((sz.diag - tail, LANE), jnp.float32)
        for i in range(0, sz.sub, 2):
            if i + 1 < sz.sub:
                other = subtile(i + 1, i + 1)
                stage[n:n + LANE, :] = jnp.where(lower, subtile(i, i), other)
                stage[tail + i // 2:tail + i // 2 + 1, :] = jnp.sum(jnp.where(equal, other, 0.0), axis=0, keepdims=True)
            else:
                stage[n:n + LANE, :] = subtile(i, i)
            n += LANE

    def same_chip(n, kept):
        m, k = n // 3, n % 3

        def halves(ref, at):
            for d in range(2):
                load(ref.at[m, pl.ds(d * sz.tile, sz.tile)], block(at + d * sz.tile, sz.tile), d)

        @pl.when(k == 0)
        def _():
            halves(a, 0)

        @pl.when((k == 2) & (kept == 0))
        def _():
            halves(lp, sz.rows)

        @pl.when(k == 1)
        def _():
            core_in(m).wait_recv()

            @pl.when(kept == 0)
            def _():
                load(a.at[m], block(0), 2)
                loaded(block(0), 2)

            load(lp.at[m], block(sz.rows), 3)
            loaded(block(sz.rows), 3)

            def middle(i):
                product(i // 2 * sz.tile + (1 - x) * sz.rows, i % 2 * sz.tile + x * sz.rows, sz.tile)
                put_strips()
                rows = pl.ds(pl.multiple_of(i * sz.full, LANE), sz.full)
                store(stage.at[pl.ds(0, sz.full)], psm.at[m, rows])
                send_mid(m, rows).start()

            loop(0, 4, middle)

        @pl.when(k != 1)
        def _():
            which = k // 2
            base = which * sz.rows

            def leave(lo, size):
                rows = pl.ds(pl.multiple_of(lo, 8), size)

                @pl.when(n == 3 * layers - 1)
                def _():
                    store(stage.at[pl.ds(0, size)], late_diag.at[rows])

                @pl.when(n < 3 * layers - 1)
                def _():
                    store(stage.at[pl.ds(0, size)], psd.at[which, m, rows])
                    send_diag(which, m, rows).start()

            def diagonal(d):
                @pl.when((k == 0) | (kept == 0))
                def _():
                    loaded(block(base + d * sz.tile, sz.tile), d)

                product(base + d * sz.tile, base + d * sz.tile, sz.tile)
                put_diag()
                leave(d * sz.diag, sz.diag)

            loop(0, 2, diagonal)
            product(base + sz.tile, base, sz.tile)
            put_strips()
            leave(2 * sz.diag, sz.full)

    def relay(q, u, size):
        x_in(q, u, size).wait_recv()
        core_r(q, u, size).start()

    def cross(q, u, size):
        j, width = u // units, size * LANE

        @pl.when(x == 0)
        def _():
            @pl.when(home & (u % units == 0))
            def _():
                core_in(j).wait_recv()

            load(a.at[j], block(c * sz.rows), 0)
            load(lp.at[j], block((1 - c) * sz.rows), 1)
            x_in(q, u, size).wait_recv()
            load(rows_of(r, u, size), block(2 * sz.rows, width), 2)
            loaded(block(c * sz.rows), 0)
            loaded(block((1 - c) * sz.rows), 1)
            loaded(block(2 * sz.rows, width), 2)

            def one(n):
                product(n * sz.tile, 2 * sz.rows, width)
                for s in range(size):
                    rows = pl.ds(pl.multiple_of(n % 2 * sz.tile, LANE), sz.tile)
                    cross_stage[s, n // 2, rows, :] = acc[:, s * LANE:(s + 1) * LANE]

            loop(0, 4, one)

        @pl.when(x == 1)
        def _():
            load(a.at[half + j], block(2 * sz.rows), 0)
            load(rows_of(r, u, size), block(c * width, width), 1)
            core_r(q, u, size).wait_recv()
            load(rows_of(rp, u, size), block((1 - c) * width, width), 2)
            loaded(block(2 * sz.rows), 0)
            loaded(block(c * width, width), 1)
            loaded(block((1 - c) * width, width), 2)

            def one(t):
                product(2 * sz.rows + t * sz.tile, 0, 2 * width)
                for i in range(2):
                    for s in range(size):
                        rows = pl.ds(pl.multiple_of(t * sz.tile, LANE), sz.tile)
                        cross_stage[s, i, rows, :] = acc[:, i * width + s * LANE:i * width + (s + 1) * LANE]

            loop(0, 2, one)

        store(cross_stage.at[pl.ds(0, size)], pc.at[pl.ds(u, size)])
        send_part(q, u, size).start()

    def add(q, u, size):
        mine, theirs = ba.at[pl.ds(0, size)], bb.at[pl.ds(0, size)]
        load(pc.at[pl.ds(u, size), y], mine, 0)
        send_part(q, u, size).wait_recv()
        load(rb.at[pl.ds(u, size)], theirs, 1)
        loaded(mine, 0)
        loaded(theirs, 1)
        ba[:size] += bb[:size]
        over = u - sz.early_units

        @pl.when(home | (over < 0))
        def _():
            store(mine, co.at[x, pl.ds(u, size), y])
            send_sum(q, u, size).start()

        @pl.when(away & (over >= 0) & (over < sz.late))
        def _():
            store(mine, late_lo.at[pl.ds(over, size)])

        @pl.when(away & (over >= sz.late))
        def _():
            store(mine, late_hi.at[pl.ds(over - sz.late, size)])

    def pass_on(q, u, size):
        from_x(q, u, size).wait_recv()
        forward(q, u, size).start()

    barrier = pltpu.get_barrier_semaphore()
    for where in (to_x, to_core, to_y):
        pl.semaphore_signal(barrier, inc=1, device_id=where, device_id_type=MESH)
    pl.semaphore_wait(barrier, 3)

    @pl.when(home)
    def _():
        loop(0, layers, lambda m: core_in(m).start())

    @pl.when(away & (x == 0))
    def _():
        loop(0, half, lambda m: core_in(m).start())

    steps = [sized(lambda *chunk: x_in(*chunk).start()), sized(relay), sized(cross), sized(add), sized(pass_on)]
    words = plan_words()

    def word(n, done):
        code = jnp.int32(0)
        for device, row in enumerate(words):
            for k, value in enumerate(row):
                code = jnp.where((g == device) & (n == k), value, code)

        def digit(_, carry):
            code, done = carry[0], list(carry[1:])
            now = code % 8
            for k, step in enumerate(steps):
                pl.when(now == k + 1)(functools.partial(step, done[k]))
                done[k] += jnp.where(now == k + 1, 1, 0)
            pl.when(now > len(steps))(functools.partial(same_chip, done[-1], now - len(steps) - 1))
            done[-1] += jnp.where(now > len(steps), 1, 0)
            return (code // 8, *done)

        return lax.fori_loop(0, WORD, digit, (code, *done))[1:]

    lax.fori_loop(0, len(words[0]), word, (jnp.int32(0),) * (len(steps) + 1))

    @pl.when(home)
    def _():
        loop(0, layers, lambda m: core_in(m).wait_send())

        def end(q, u, size):
            send_sum(q, u, size).wait_recv()

            @pl.when(u < sz.early_units)
            def _():
                forward(q, u, size).wait_recv()
                forward(q, u, size).wait_send()

        loop(0, sz.chunks, sized(end))

    @pl.when(away & (x == 0))
    def _():
        loop(0, half, lambda m: core_in(m).wait_send())

    @pl.when(x == 1)
    def _():
        loop(0, sz.chunks, sized(lambda *chunk: core_r(*chunk).wait_send()))

    @pl.when(away)
    def _():
        def end(m):
            send_diag(0, m).wait()
            send_mid(m).wait()

            @pl.when(m < layers - 1)
            def _():
                send_diag(1, m).wait()

        loop(0, layers, end)

    def sent(q, u, size):
        x_in(q, u, size).wait_send()
        send_part(q, u, size).wait_send()

        @pl.when(home | (u < sz.early_units))
        def _():
            send_sum(q, u, size).wait_send()

    loop(0, sz.chunks, sized(sent))


def exchange(sz, a):
    f32, bf16 = jnp.float32, jnp.bfloat16
    dma = pltpu.SemaphoreType.DMA
    rows = (sz.rows, sz.cols)
    strip = (sz.rows, LANE)
    most = max(size for _, size in SPLIT)
    outs = [
        ((sz.half,) + rows, bf16),
        ((sz.layers,) + rows, bf16),
        ((sz.half,) + rows, bf16),
        ((2, sz.layers, sz.own, LANE), f32),
        ((sz.layers, sz.mid, LANE), f32),
        ((2, sz.layers, sz.own, LANE), f32),
        ((sz.layers, sz.mid, LANE), f32),
        ((sz.all_units, 2) + strip, f32),
        ((sz.all_units,) + strip, f32),
        ((2, sz.all_units, 2) + strip, f32),
        ((sz.own, LANE), f32),
        ((sz.late,) + strip, f32),
        ((sz.late,) + strip, f32),
    ]
    n, q = sz.layers, sz.chunks
    res = pl.pallas_call(
        functools.partial(exchange_kernel, sz),
        name="exchange",
        out_shape=[jax.ShapeDtypeStruct(s, d) for s, d in outs],
        in_specs=[pl.BlockSpec(memory_space=pl.ANY)],
        out_specs=[pl.BlockSpec(memory_space=pl.ANY)] * len(outs),
        scratch_shapes=[
            pltpu.VMEM((3 * sz.rows, sz.cols), bf16),
            pltpu.VMEM((sz.tile, sz.tile), f32),
            pltpu.VMEM((sz.full, LANE), f32),
            pltpu.VMEM((most, 2) + strip, f32),
            pltpu.VMEM((most,) + strip, f32),
            pltpu.VMEM((most,) + strip, f32),
            dma((5,)), dma((q,)), dma((q,)), dma((n,)), dma((n,)), dma((q,)), dma((q,)),
            dma((3, n)), dma((3, n)), dma((q,)), dma((q,)), dma((q,)), dma((3, q)), dma((q,)),
        ],
        compiler_params=pltpu.CompilerParams(collective_id=0, has_side_effects=True, vmem_limit_bytes=60 * 2**20),
    )(a)
    return (res[3], res[5], res[4], res[6], res[9]), res[10:]


OUTS = 5
INS = 6
DIAGS = 4
ZERO_ROWS = 256
HOME_PARTS = (0, 0, 4, 9, 14)
AWAY_PARTS = (0, 3, 5, 7, 8)


class Blocks:
    def __init__(self, sz, out, ob, out_sem):
        self.sz, self.out, self.ob, self.out_sem = sz, out, ob, out_sem
        self.lower, self.equal = triangles()

    def put(self, b, i, k, value):
        def at(n):
            return pl.ds(n * LANE if isinstance(n, int) else pl.multiple_of(n * LANE, LANE), LANE)

        self.ob[b, at(i), at(k)] = value

    def free(self, n):
        @pl.when(n >= OUTS)
        def _():
            self.done(n % OUTS)

    def leave(self, n, slot, m):
        b = n % OUTS
        pltpu.make_async_copy(self.ob.at[b], self.out.at[slot, m], self.out_sem.at[b]).start()

    def done(self, b):
        pltpu.make_async_copy(self.ob.at[b], self.out.at[0, 0], self.out_sem.at[b]).wait()

    def drain(self, count):
        for b in range(min(OUTS, count)):
            self.done(b)

    def unit(self, b, u, strip, transposed):
        count = 2 * self.sz.sub

        @pl.when(transposed)
        def _():
            for k in range(count):
                self.put(b, u, k, strip(k).T)

        @pl.when(jnp.logical_not(transposed))
        def _():
            for k in range(count):
                self.put(b, k, u, strip(k))

    def diagonal(self, b, total):
        sz, sub = self.sz, self.sz.sub
        for e in range(2):
            row, first = e * sz.diag, e * sub
            tail = row + (sz.low + sz.pairs) * LANE
            for i in range(sub):
                for k in range(i):
                    s = total(row, LANE)
                    self.put(b, first + i, first + k, s)
                    self.put(b, first + k, first + i, s.T)
                    row += LANE
            for i in range(0, sub, 2):
                s = total(row, LANE)
                flip = s.T
                self.put(b, first + i, first + i, jnp.where(self.lower, s, flip))
                if i + 1 < sub:
                    line = jnp.broadcast_to(total(tail + i // 2, 1), (LANE, LANE))
                    other = jnp.where(self.equal, line, jnp.where(self.lower, flip, s))
                    self.put(b, first + i + 1, first + i + 1, other)
                row += LANE
        for k in range(sub):
            for i in range(sub):
                s = total(2 * sz.diag + k * sz.tile + i * LANE, LANE)
                self.put(b, sub + i, k, s)
                self.put(b, k, sub + i, s.T)


def assemble_kernel(sz, number, *refs):
    late_mine = late_theirs = None
    role, psd, rsd, psm, rsm, co = refs[:6]
    if AWAY_PARTS[number + 1] == sz.layers:
        late_mine, late_theirs = refs[6:8]
    out = refs[-9]
    ob, ib, db, zeros, out_sem, in_sem, diag_sem, zero_sem = refs[-8:]
    layers, half, units, sub, t = sz.layers, sz.half, sz.units, sz.sub, sz.tile
    x = role[1]
    blocks = Blocks(sz, out, ob, out_sem)

    @pl.when(role[0] == 0)
    def _():
        lo, hi = HOME_PARTS[number:number + 2]
        first = lo == 0 and hi > 0
        per = sz.rows // ZERO_ROWS

        def zero(n):
            rows = pl.ds(pl.multiple_of(n % per * ZERO_ROWS, ZERO_ROWS), ZERO_ROWS)
            return pltpu.make_async_copy(zeros, out.at[2, n // per, rows], zero_sem)

        def place(n):
            over = jnp.where(n >= layers, 1, 0)
            return x + over - 2 * x * over, n // 2 - over * half, n % 2

        def fetch(n):
            side, j, slot = place(n)
            b = (n - lo) % INS
            return pltpu.make_async_copy(co.at[side, pl.ds(j * units, units), slot], ib.at[b], in_sem.at[b])

        loop(lo, min(lo + INS, hi), lambda n: fetch(n).start())
        if first:
            zeros[...] = jnp.zeros_like(zeros)
            loop(0, layers * per, lambda n: zero(n).start())

        def one(n):
            side, j, slot = place(n)
            k = n - lo
            fetch(n).wait()
            blocks.free(k)

            def unit(u):
                blocks.unit(k % OUTS, u, lambda i: ib[k % INS, u, i * LANE:(i + 1) * LANE, :], side == 0)

            loop(0, units, unit)
            blocks.leave(k, slot, side * half + j)

            @pl.when(n + INS < hi)
            def _():
                fetch(n + INS).start()

        loop(lo, hi, one)
        blocks.drain(hi - lo)
        if first:
            loop(0, layers * per, lambda n: zero(n).wait())

    @pl.when(role[0] == 1)
    def _():
        lo, hi = AWAY_PARTS[number:number + 2]
        depth, diag_depth = INS // 2, DIAGS // 2

        def fetch_diag(d, go):
            for ref, late, k in ((psd, late_mine, 0), (rsd, late_theirs, 1)):
                b = 2 * ((d - 2 * lo) % diag_depth) + k
                if late is None:
                    go(pltpu.make_async_copy(ref.at[d % 2, d // 2], db.at[b], diag_sem.at[b]))
                else:
                    @pl.when(d == 2 * layers - 1)
                    def _():
                        go(pltpu.make_async_copy(late, db.at[b], diag_sem.at[b]))

                    @pl.when(d < 2 * layers - 1)
                    def _():
                        go(pltpu.make_async_copy(ref.at[d % 2, d // 2], db.at[b], diag_sem.at[b]))

        def fetch_mid(m, go):
            for ref, k in ((psm, 0), (rsm, 1)):
                b = 2 * ((m - lo) % depth) + k
                go(pltpu.make_async_copy(ref.at[m], ib.at[b], in_sem.at[b]))

        def start(c):
            c.start()

        def wait(c):
            c.wait()

        loop(2 * lo, 2 * lo + diag_depth, lambda d: fetch_diag(d, start))
        loop(lo, min(lo + depth, hi), lambda m: fetch_mid(m, start))

        def one(m):
            def side(k):
                d, n = 2 * m + k, 3 * (m - lo) + k
                mine = 2 * ((d - 2 * lo) % diag_depth)
                fetch_diag(d, wait)
                blocks.free(n)
                blocks.diagonal(n % OUTS, lambda row, size: db[mine, row:row + size, :] + db[mine + 1, row:row + size, :])
                blocks.leave(n, 2 * (x + k - 2 * x * k), m)

                @pl.when(d + diag_depth < 2 * hi)
                def _():
                    fetch_diag(d + diag_depth, start)

            loop(0, 2, side)
            n = 3 * (m - lo) + 2
            mine = 2 * ((m - lo) % depth)
            fetch_mid(m, wait)
            blocks.free(n)

            def strips(u):
                tile, col = u // sub, u % sub
                for i in range(sub):
                    rows = pl.ds(pl.multiple_of(u % 2 * t + i * LANE, LANE), LANE)
                    s = ib[mine, u // 2, rows, :] + ib[mine + 1, u // 2, rows, :]
                    blocks.put(n % OUTS, tile // 2 * sub + i, tile % 2 * sub + col, s)

            loop(0, 4 * sub, strips)
            blocks.leave(n, 1, m)

            @pl.when(m + depth < hi)
            def _():
                fetch_mid(m + depth, start)

        loop(lo, hi, one)
        blocks.drain(3 * (hi - lo))


def assemble(sz, number, role, parts, late=(), out=None):
    f32, dma = jnp.float32, pltpu.SemaphoreType.DMA
    block = (sz.units, sz.rows, LANE)
    hbm = pl.BlockSpec(memory_space=pl.ANY)
    psd, rsd, psm, rsm, co = parts
    args = [role, psd, rsd, psm.reshape((-1,) + block), rsm.reshape((-1,) + block), co, *late]
    if out is not None:
        args.append(out)
    moved = sz.layers * sz.rows * sz.rows * 4 * 2
    return pl.pallas_call(
        functools.partial(assemble_kernel, sz, number),
        out_shape=jax.ShapeDtypeStruct((3, sz.layers, sz.rows, sz.rows), f32),
        in_specs=[pl.BlockSpec(memory_space=pltpu.SMEM)] + [hbm] * (len(args) - 1),
        out_specs=hbm,
        scratch_shapes=[
            pltpu.VMEM((OUTS, sz.rows, sz.rows), f32),
            pltpu.VMEM((INS,) + block, f32),
            pltpu.VMEM((DIAGS, sz.own, LANE), f32),
            pltpu.VMEM((ZERO_ROWS, sz.rows), f32),
            dma((OUTS,)), dma((INS,)), dma((DIAGS,)), dma,
        ],
        input_output_aliases={} if out is None else {len(args) - 1: 0},
        cost_estimate=pl.CostEstimate(flops=10**10, bytes_accessed=moved, transcendentals=0),
        compiler_params=pltpu.CompilerParams(vmem_limit_bytes=60 * 2**20),
    )(*args)


def finish_kernel(sz, last, role, *refs):
    count = 1 if last else 3
    pieces, co, out = refs[:count], refs[count], refs[count + 2]
    ob, ib, hb, out_sem, in_sem, head_sem = refs[-6:]
    side = 1 - role[1]
    m = side * sz.half + sz.half - 1
    slots = role[2], 1 - role[2]
    tail = sz.lead + sz.late
    blocks = Blocks(sz, out, ob, out_sem)

    @pl.when(role[0] == 0)
    def _():
        def heads(b):
            first = (sz.half - 1) * sz.units
            return pltpu.make_async_copy(co.at[side, pl.ds(first, sz.lead), slots[b]], hb.at[b], head_sem.at[b])

        copies = [pltpu.make_async_copy(ref, ib.at[n], in_sem.at[n]) for n, ref in enumerate(pieces)]
        for c in copies:
            c.start()

        def head(b):
            heads(b).wait()
            loop(0, sz.lead, lambda u: blocks.unit(b, u, lambda k: hb[b, u, k * LANE:(k + 1) * LANE, :], side == 0))

        def units(n, b, first):
            copies[n].wait()
            loop(0, sz.late, lambda u: blocks.unit(b, first + u, lambda k: ib[n, u, k * LANE:(k + 1) * LANE, :], side == 0))

        def part(b, first, size, go):
            rows = pl.ds(first * LANE, size * LANE)

            @pl.when(side == 0)
            def _():
                go(pltpu.make_async_copy(ob.at[b, rows], out.at[slots[b], m, rows], out_sem.at[b]))

            @pl.when(side == 1)
            def _():
                go(pltpu.make_async_copy(ob.at[b, :, rows], out.at[slots[b], m, :, rows], out_sem.at[b]))

        def start(c):
            c.start()

        def wait(c):
            c.wait()

        if last:
            units(0, 1, tail)
            part(1, tail, sz.late, start)
            part(1, tail, sz.late, wait)
        else:
            heads(0).start()
            heads(1).start()
            head(0)
            units(0, 0, sz.lead)
            units(1, 0, tail)
            blocks.leave(0, slots[0], m)
            head(1)
            units(2, 1, sz.lead)
            part(1, 0, tail, start)
            blocks.done(0)
            part(1, 0, tail, wait)


def finish(sz, last, role, pieces, co, out):
    f32, dma = jnp.float32, pltpu.SemaphoreType.DMA
    count = len(pieces)
    hbm = pl.BlockSpec(memory_space=pl.ANY)
    return pl.pallas_call(
        functools.partial(finish_kernel, sz, last),
        name="finish_last" if last else "finish",
        out_shape=jax.ShapeDtypeStruct(out.shape, f32),
        in_specs=[pl.BlockSpec(memory_space=pltpu.SMEM)] + [hbm] * (count + 2),
        out_specs=hbm,
        scratch_shapes=[
            pltpu.VMEM((2, sz.rows, sz.rows), f32),
            pltpu.VMEM((count, sz.late, sz.rows, LANE), f32),
            pltpu.VMEM((2, sz.lead, sz.rows, LANE), f32),
            dma((2,)), dma((count,)), dma((2,)),
        ],
        input_output_aliases={count + 2: 0},
        cost_estimate=pl.CostEstimate(flops=3 * 10**9, bytes_accessed=8 * sz.rows * sz.rows, transcendentals=0),
        compiler_params=pltpu.CompilerParams(vmem_limit_bytes=32 * 2**20),
    )(role, *pieces, co, out)


def solution(mesh):
    width = mesh.shape["g"]
    axes = ("kk", "g")

    def pairs(moves):
        return [(a * width + b, c * width + d) for (a, b), (c, d) in moves]

    ys = range(mesh.shape["kk"])
    over_x = pairs([((y, g), (y, (g + 2) % 4)) for y in ys for g in (0, 3)])
    away_y = pairs([((y, g), (1 - y, g)) for y in ys for g in (0, 3)])
    home_y = pairs([((y, g), (1 - y, g)) for y in ys for g in (1, 2)])

    def local_part(a_loc):
        sz = Sizes(*a_loc.shape)
        g = lax.axis_index("g")
        x, c = g // 2, g % 2
        role = jnp.stack([jnp.where(c == x, 1, 0), x, lax.axis_index("kk")]).astype(jnp.int32)
        parts, (late_diag, late_lo, late_hi) = exchange(sz, a_loc)
        lo = lax.ppermute(late_lo, axes, over_x)
        hi = lax.ppermute(late_hi, axes, over_x)
        theirs = lax.ppermute(late_diag, axes, away_y)
        lo_too = lax.ppermute(lo, axes, home_y)
        hi_too = lax.ppermute(hi, axes, home_y)
        out = assemble(sz, 0, role, parts)
        out = assemble(sz, 1, role, parts, (), out)
        out = assemble(sz, 2, role, parts, (), out)
        out = assemble(sz, 3, role, parts, (late_diag, theirs), out)
        out = finish(sz, False, role, (lo, hi, lo_too), parts[-1], out)
        out = finish(sz, True, role, (hi_too,), parts[-1], out)
        return out[None]

    return jax.shard_map(local_part, mesh=mesh, in_specs=(P(None, ("m", "g"), "kk"),), out_specs=P(("m", "g"), None, None, None, None), check_vma=False)
```
